64 devices in a mesh: dp: 4 (over x, y), pp: 16 (over z, core).
Axes of the slice: x: 2, y: 2, z: 8, core: 2. Of those that a mesh axis runs over, the one named last changes fastest.
The devices are a block of a 4x4x8 slice.
Arguments:
- hidden: bfloat16 [128, 512, 576], P(('dp', 'pp')), parts along dimension 0
- labels: int32 [128, 512], P(('dp', 'pp')), parts along dimension 0
- gamma: float32 [576], replicated
- table: bfloat16 [49152, 576], P('pp')
Outputs:
- output 1: float32 [128, 512], P(('dp', 'pp')), parts along dimension 0
- output 2: bfloat16 [128, 512, 576], P(('dp', 'pp')), parts along dimension 0
- output 3: float32 [4], P('dp'), parts along dimension 0
- output 4: float32 [196608, 576], P(('dp', 'pp')), parts along dimension 0
- output 5: float32 [2304], P('dp'), parts along dimension 0
There are 4 independent parts. The reference program is written for one: setup_inputs(seed, part) draws one part's arguments, and reference() takes and returns one part's arrays. A program takes and returns all parts, laid end to end along the dimension named above; an argument that names none is the same for every part.
All inputs are finite; a program needn't handle non-finite values.
Results may differ from the reference program's by a relative error of at most 0.001.
Values are sent between devices in bfloat16 or wider.
A program may use at most 768 MiB of HBM per device.

```python
import jax
import jax.numpy as jnp
from jax import lax

MICROBATCHES = 32
SEQ_LEN = 512
D_MODEL = 576
VOCAB_SIZE = 49152
SOFT_CAP = 30
EPS = 1e-6
LOGIT_SCALE = 10.0


def setup_inputs(seed: int = 0, part: int = 0) -> dict:
    base_key = jax.random.key(seed)
    shared_key, part_base = jax.random.split(base_key)
    part_key = jax.random.fold_in(part_base, part)
    key_hidden, key_labels = jax.random.split(part_key)
    key_gain, key_table = jax.random.split(shared_key)
    hidden = jax.random.normal(key_hidden, (MICROBATCHES, SEQ_LEN, D_MODEL), jnp.float32).astype(jnp.bfloat16)
    labels = jax.random.randint(key_labels, (MICROBATCHES, SEQ_LEN), 0, VOCAB_SIZE, dtype=jnp.int32)
    gamma = 0.3 * jax.random.normal(key_gain, (D_MODEL,), jnp.float32)
    table_f = jax.random.normal(key_table, (VOCAB_SIZE, D_MODEL), jnp.float32) * (LOGIT_SCALE * D_MODEL ** -0.5)
    return {'hidden': hidden, 'labels': labels, 'gamma': gamma, 'table': table_f.astype(jnp.bfloat16)}


def norm_rows(rows, gain):
    mean_sq = jnp.mean(rows * rows, axis=-1, keepdims=True)
    return rows * lax.rsqrt(mean_sq + EPS) * (1.0 + gain)


def reference(hidden, labels, gamma, table):
    total = MICROBATCHES * SEQ_LEN
    vocab_ids = lax.broadcasted_iota(jnp.int32, (1, VOCAB_SIZE), 1)

    def micro_step(carry, scan_in):
        grad_table, grad_gain = carry
        block, block_labels = scan_in
        normed32, norm_vjp = jax.vjp(norm_rows, block.astype(jnp.float32), gamma)
        normed = normed32.astype(jnp.bfloat16)
        logits = jnp.dot(normed, table.T, preferred_element_type=jnp.float32)
        tanh_z = jnp.tanh(logits / SOFT_CAP)
        capped = SOFT_CAP * tanh_z
        row_max = jnp.max(capped, axis=1, keepdims=True)
        log_norm = row_max + jnp.log(jnp.sum(jnp.exp(capped - row_max), axis=1, keepdims=True))
        label_hit = vocab_ids == block_labels[:, None]
        label_logit = jnp.sum(jnp.where(label_hit, capped, 0.0), axis=1)
        tok_loss = log_norm[:, 0] - label_logit
        soft_probs = jnp.exp(capped - log_norm)
        grad_capped = jnp.where(label_hit, soft_probs - 1.0, soft_probs) / total
        grad_logits = (grad_capped * (1.0 - tanh_z * tanh_z)).astype(jnp.bfloat16)
        grad_normed = jnp.dot(grad_logits, table, preferred_element_type=jnp.float32)
        grad_block, gain_part = norm_vjp(grad_normed)
        table_part = jnp.dot(grad_logits.T, normed, preferred_element_type=jnp.float32)
        return (grad_table + table_part, grad_gain + gain_part), (tok_loss, grad_block.astype(jnp.bfloat16))

    init_acc = (jnp.zeros((VOCAB_SIZE, D_MODEL), jnp.float32), jnp.zeros((D_MODEL,), jnp.float32))
    (grad_table, grad_gain), (tok_loss, grad_hidden) = lax.scan(micro_step, init_acc, (hidden, labels))
    mean_loss = jnp.reshape(jnp.mean(tok_loss), (1,))
    return tok_loss, grad_hidden, mean_loss, grad_table, grad_gain
```

```python
import functools
import math

import jax
import jax.numpy as jnp
from jax import lax
from jax.experimental import pallas as pl
from jax.experimental.pallas import tpu as pltpu
from jax.sharding import PartitionSpec as P

F32, BF16 = jnp.float32, jnp.bfloat16
SOFT_CAP = 30.0
EXP2_SCALE = SOFT_CAP * math.log2(math.e)
MESH = pl.DeviceIdType.MESH
TILE = 256
TB = 2 * TILE
CH = 256
FR = 192
PAD_ROWS = 8
VC = 3072
VB = 3072
Q = (0, 1)


def lanes(q):
    return pl.ds(q * TILE, TILE)


def run_stream(items, ahead):
    vals = {}
    for i in range(len(items) + ahead):
        if i < len(items):
            vals[i] = items[i][0]()
        if i >= ahead:
            items[i - ahead][1](vals.pop(i - ahead))


def kernel(n_pp, nb, per, total, V, D, n_hbm, lab, W, WT, dW_in, dn_hbm, dW_out, s_out,
           U, nbuf, dW, dnb, labm, svec, own, rbuf,
           n_sem, o_sem, w_sem, send_sem, recv_sem):
    tc = n_hbm.shape[2]
    me = lax.axis_index("pp")

    def peer(k):
        return {"pp": lax.rem(me + k, n_pp)}

    def n_copies(i):
        slot = lax.rem(i, 3)
        return [pltpu.make_async_copy(n_hbm.at[i * per + a],
                                      nbuf.at[slot, :, pl.ds(a * tc, tc)], n_sem.at[slot, a])
                for a in range(per)]

    def dn_copies(i):
        slot = lax.rem(i, 2)
        return [pltpu.make_async_copy(dnb.at[slot, :, pl.ds(a * tc, tc)],
                                      dn_hbm.at[i * per + a], o_sem.at[slot, a])
                for a in range(per)]

    def stat_copy(i, k):
        return pltpu.make_async_remote_copy(
            src_ref=own.at[i], dst_ref=rbuf.at[i, me], send_sem=send_sem.at[i, k - 1],
            recv_sem=recv_sem.at[i, n_pp - 1 - k], device_id=peer(k), device_id_type=MESH)

    w_load = pltpu.make_async_copy(dW_in, dW, w_sem)
    w_load.start()
    for c in n_copies(0):
        c.start()
    if n_pp > 1:
        barrier = pltpu.get_barrier_semaphore()
        for k in range(1, n_pp):
            pl.semaphore_signal(barrier, inc=1, device_id=peer(k), device_id_type=MESH)
        pl.semaphore_wait(barrier, n_pp - 1)
    base = me * V

    def f_part(slot, nF, c, st):
        rows = pl.ds(pl.multiple_of(c * VC, VC), VC)
        z = jnp.dot(W[rows, :], nF[...], preferred_element_type=F32)
        t = jnp.tanh(z * (1.0 / SOFT_CAP))
        U[slot, rows, :] = t
        return st + jnp.sum(jnp.exp2(t * EXP2_SCALE).reshape(VC // 8, 8, TB), axis=0)

    def b_part(slot, nB, c, tl):
        rows = pl.ds(pl.multiple_of(c * VB, VB), VB)
        t = U[slot, rows, :]
        p = jnp.exp2(t * EXP2_SCALE) * svec[0:1, :]
        hit = lax.broadcasted_iota(jnp.int32, (VB, TB), 0) == labm[0:1, :] - c * VB
        tl = tl + jnp.sum(jnp.where(hit, t, 0.0).reshape(VB // 8, 8, TB), axis=0)
        g = p - jnp.where(hit, 1.0 / total, 0.0)
        dz = (g * (1.0 - t * t)).astype(BF16)
        return dz, tl

    def b_dots(slot, nB, c, dz):
        part = jnp.dot(WT[:, pl.ds(pl.multiple_of(c * VB, VB), VB)], dz, preferred_element_type=F32)
        cols = pl.ds(pl.multiple_of(c * VB, VB), VB)
        dW[:, cols] += lax.dot_general(nB[...], dz, (((1,), (1,)), ((), ())), preferred_element_type=F32)
        return part

    def fwd_start(i):
        for c in n_copies(i):
            c.wait()

        @pl.when(i + 1 < nb)
        def _():
            for c in n_copies(i + 1):
                c.start()

    def fwd_end(i, st):
        own[i] = jnp.sum(st, axis=0, keepdims=True)
        for k in range(1, n_pp):
            stat_copy(i, k).start()

    def bwd_start(i):
        for k in range(1, n_pp):
            stat_copy(i, k).wait_recv()
        acc = jnp.zeros((1, TB), F32)
        for k in range(n_pp):
            acc = acc + (jnp.where(k == me, own[i], rbuf[i, k]) if n_pp > 1 else own[i])
        s_out[i] = acc
        svec[...] = jnp.broadcast_to(1.0 / (acc * total), (8, TB))
        labm[...] = jnp.broadcast_to(lab[i] - base, (8, TB))

        @pl.when(i >= 2)
        def _():
            for c in dn_copies(i - 2):
                c.wait()

    def bwd_end(i, tl):
        dnb[lax.rem(i, 2), pl.ds(D, PAD_ROWS), :] = tl
        for c in dn_copies(i):
            c.start()
        for k in range(1, n_pp):
            stat_copy(i, k).wait_send()

    z8 = jnp.zeros((8, TB), F32)

    def step(i, _):
        @pl.when(i < nb)
        def _():
            fwd_start(i)
            slot, nF = lax.rem(i, 2), nbuf.at[lax.rem(i, 3)]
            st = lax.fori_loop(0, V // VC, lambda c, st: f_part(slot, nF, c, st), z8)
            fwd_end(i, st)

        @pl.when(i == 0)
        def _():
            w_load.wait()

        @pl.when(i > 0)
        def _():
            bwd_start(i - 1)
            slot, nB = lax.rem(i - 1, 2), nbuf.at[lax.rem(i - 1, 3)]
            dn = dnb.at[slot]

            def body(c, tl):
                dz, tl = b_part(slot, nB, c, tl)
                part = b_dots(slot, nB, c, dz)
                @pl.when(c == 0)
                def _():
                    dn[0:D, :] = part

                @pl.when(c > 0)
                def _():
                    dn[0:D, :] += part
                return tl
            if V // VB == 1:
                dz, tl = b_part(slot, nB, 0, z8)
                dn[0:D, :] = b_dots(slot, nB, 0, dz)
            else:
                dn[...] = jnp.zeros((D + PAD_ROWS, TB), F32)
                def body2(c, tl):
                    dz, tl = b_part(slot, nB, c, tl)
                    dn[0:D, :] += b_dots(slot, nB, c, dz)
                    return tl
                tl = lax.fori_loop(0, V // VB, body2, z8)
            bwd_end(i - 1, tl)
        return 0
    lax.fori_loop(0, nb + 1, step, 0)
    w_store = pltpu.make_async_copy(dW, dW_out, w_sem)
    w_store.start()
    for i in (nb - 2, nb - 1):
        for c in dn_copies(i):
            c.wait()
    w_store.wait()


def chunk_call(n_all, lab, W, WT, dW, *, n_pp, total, cid):
    D, V = WT.shape
    g, _, tc = n_all.shape
    per = TB // tc
    nb = g // per
    hbm = pl.BlockSpec(memory_space=pl.ANY)
    vmem = pl.BlockSpec(memory_space=pltpu.VMEM)
    nk = max(n_pp - 1, 1)
    return pl.pallas_call(
        functools.partial(kernel, n_pp, nb, per, float(total), V, D),
        out_shape=[jax.ShapeDtypeStruct((g, D + PAD_ROWS, tc), F32), jax.ShapeDtypeStruct((D, V), F32),
                   jax.ShapeDtypeStruct((nb, 1, TB), F32)],
        in_specs=[hbm, vmem, vmem, vmem, hbm],
        out_specs=[hbm, hbm, vmem],
        scratch_shapes=[
            pltpu.VMEM((2, V, TB), F32),
            pltpu.VMEM((3, D, TB), BF16), pltpu.VMEM((D, V), F32), pltpu.VMEM((2, D + PAD_ROWS, TB), F32),
            pltpu.VMEM((8, TB), jnp.int32), pltpu.VMEM((8, TB), F32),
            pltpu.VMEM((nb, 1, TB), F32), pltpu.VMEM((nb, n_pp, 1, TB), F32),
            pltpu.SemaphoreType.DMA((3, per)), pltpu.SemaphoreType.DMA((2, per)), pltpu.SemaphoreType.DMA,
            pltpu.SemaphoreType.DMA((nb, nk)), pltpu.SemaphoreType.DMA((nb, nk)),
        ],
        input_output_aliases={4: 1},
        compiler_params=pltpu.CompilerParams(
            vmem_limit_bytes=56 * 1024 * 1024,
            **(dict(collective_id=cid, has_side_effects=True) if n_pp > 1 else {})),
        cost_estimate=pl.CostEstimate(flops=6 * g * tc * D * V, bytes_accessed=g * tc * D * 6 + D * V * 8, transcendentals=0),
        name=f"core{cid}",
    )(n_all, lab, W, WT, dW)


def sum_kernel(n_pp, x_ref, o_ref, rbuf, send_sem, recv_sem):
    me = lax.axis_index("pp")

    def peer(k):
        return {"pp": lax.rem(me + k, n_pp)}

    barrier = pltpu.get_barrier_semaphore()
    for k in range(1, n_pp):
        pl.semaphore_signal(barrier, inc=1, device_id=peer(k), device_id_type=MESH)
    pl.semaphore_wait(barrier, n_pp - 1)
    copies = [pltpu.make_async_remote_copy(
        src_ref=x_ref, dst_ref=rbuf.at[me], send_sem=send_sem.at[k - 1], recv_sem=recv_sem.at[n_pp - 1 - k],
        device_id=peer(k), device_id_type=MESH) for k in range(1, n_pp)]
    for c in copies:
        c.start()
    for c in copies:
        c.wait_recv()
    acc = jnp.zeros_like(o_ref)
    for k in range(n_pp):
        acc = acc + jnp.where(k == me, x_ref[...], rbuf[k])
    o_ref[...] = acc
    for c in copies:
        c.wait_send()


def small_sum(x, n_pp, cid):
    vmem = pl.BlockSpec(memory_space=pltpu.VMEM)
    return pl.pallas_call(
        functools.partial(sum_kernel, n_pp), out_shape=jax.ShapeDtypeStruct(x.shape, F32),
        in_specs=[vmem], out_specs=vmem,
        scratch_shapes=[pltpu.VMEM((n_pp,) + x.shape, F32), pltpu.SemaphoreType.DMA((n_pp - 1,)),
                        pltpu.SemaphoreType.DMA((n_pp - 1,))],
        compiler_params=pltpu.CompilerParams(collective_id=cid, has_side_effects=True), name="small_sum")(x)


EPS = 1e-6
WIDTHS = (256, 512, 256)


def norm_cols(cols, gain):
    mean_sq = jnp.mean(cols * cols, axis=1, keepdims=True)
    return cols * lax.rsqrt(mean_sq + EPS) * (1.0 + gain)[None, :, None]


def solution(mesh):
    n_pp = mesh.shape["pp"]

    def local_fn(hidden, labels, gamma, table):
        mb, seq, D = hidden.shape
        V = table.shape[0]
        T = mb * seq
        total = T * n_pp
        me = lax.axis_index("pp")
        cols = jnp.swapaxes(hidden, 1, 2).astype(F32)
        normed, norm_vjp = jax.vjp(norm_cols, cols, gamma)
        normed = jnp.concatenate(list(normed.astype(BF16)), axis=1)
        starts = [sum(WIDTHS[:k]) for k in range(len(WIDTHS))]
        gathered = [lax.all_gather(normed[:, a:a + w], "pp", axis=0) for a, w in zip(starts, WIDTHS)]
        all_labels = lax.all_gather(labels.reshape(T), "pp", axis=0)
        WT = table.T
        dW = jnp.zeros(WT.shape, F32)
        dn_own, sums = [], []
        for k, (a, w) in enumerate(zip(starts, WIDTHS)):
            lab = all_labels[:, a:a + w].reshape(n_pp * w // TB, 1, TB)
            dn, dW, s = chunk_call(gathered[k], lab, table, WT, dW, n_pp=n_pp, total=total, cid=k + 1)
            dn_own.append(lax.psum_scatter(dn, "pp", scatter_dimension=0, tiled=False))
            sums.append(lax.dynamic_index_in_dim(s.reshape(n_pp, w), me, 0, keepdims=False))
        dn = jnp.concatenate(dn_own, axis=1)
        loss = jnp.log(jnp.concatenate(sums)) - SOFT_CAP * jnp.sum(dn[D:], axis=0)
        d_cols, d_gain = norm_vjp(dn[:D].reshape(D, mb, seq).swapaxes(0, 1))
        flat = jnp.concatenate([d_gain, jnp.sum(loss)[None]])
        rows = -(-flat.shape[0] // 1024) * 8
        flat = jnp.pad(flat, (0, rows * 128 - flat.shape[0])).reshape(rows, 128)
        flat = small_sum(flat, n_pp, len(WIDTHS) + 1).reshape(-1)
        return (loss.reshape(mb, seq), jnp.swapaxes(d_cols, 1, 2).astype(BF16), flat[D:D + 1] / total,
                dW.T, flat[:D])

    token_spec = P(("dp", "pp"))
    return jax.shard_map(local_fn, mesh=mesh,
                         in_specs=(token_spec, token_spec, P(), P("pp")),
                         out_specs=(token_spec, token_spec, P("dp"), token_spec, P("dp")),
                         check_vma=False)
```

```python
import functools
import math

import jax
import jax.numpy as jnp
from jax import lax
from jax.experimental import pallas as pl
from jax.experimental.pallas import tpu as pltpu
from jax.sharding import PartitionSpec as P

F32, BF16 = jnp.float32, jnp.bfloat16
SOFT_CAP = 30.0
EPS = 1e-6
EXP2_SCALE = SOFT_CAP * math.log2(math.e)
MESH = pl.DeviceIdType.MESH
CORES = 2
LANE = 128
TILES = 4
TB = LANE * TILES
HALF = TB // CORES
PAD_ROWS = 8
HOPS = (4, 3)


def kernel(n_pp, total, n_own, lab_own, W, WT,
           dn_out, dW_out, s_out, n_all, dnp, prx,
           U, nblk, dW, dnb, svec, labm, lab_all, own_s, x1, x2, Sb, rx, ownv, sendb, outv,
           ag_recv, ag_send, pag_recv, pag_send, pair_recv, pair_send, dnp_sem, ring_recv, ring_send,
           st_recv, st_send, lab_recv, lab_send, nl_sem, ov_sem, io_sem):
    D, T = n_own.shape
    V = W.shape[0]
    D8 = D + PAD_ROWS
    nz = n_pp // CORES
    nsb = T // LANE
    per_sb = n_pp // TILES
    nb = nsb * per_sb
    me = lax.axis_index("pp")
    z, core = me // CORES, lax.rem(me, CORES)

    def dev(chip, c=core):
        return lax.rem(chip + 2 * nz, nz) * CORES + c

    def at(index):
        return {"pp": index}

    partner = at(z * CORES + 1 - core)

    def lanes_of(sb):
        return pl.ds(pl.multiple_of(sb * LANE, LANE), LANE)

    def remote(src, dst, ssem, rsem, where):
        return pltpu.make_async_remote_copy(src_ref=src, dst_ref=dst, send_sem=ssem, recv_sem=rsem,
                                            device_id=where, device_id_type=MESH)

    def sign(sb, d):
        g = 1 - 2 * lax.rem(sb, 2)
        return g if d == 0 else -g

    def ag_ring(sb, d, r):
        g = sign(sb, d)
        if r == 0:
            src = n_own.at[:, lanes_of(sb)]
        else:
            src = n_all.at[dev(z - g * r), :, lanes_of(sb)]
        return remote(src, n_all.at[dev(z - g * r), :, lanes_of(sb)], ag_send.at[sb, d, r], ag_recv.at[sb, d, r],
                      at(dev(z + g)))

    def ag_partner(sb, chip, own=False):
        i = lax.rem(chip + 2 * nz, nz)
        src = n_own.at[:, lanes_of(sb)] if own else n_all.at[dev(chip), :, lanes_of(sb)]
        return remote(src, n_all.at[dev(chip), :, lanes_of(sb)], pag_send.at[sb, i], pag_recv.at[sb, i], partner)

    def ag_first(sb):
        for d in (0, 1):
            ag_ring(sb, d, 0).start()
        ag_partner(sb, z, own=True).start()

    def ag_next(sb, r):
        for d in (0, 1):
            if r <= HOPS[d]:
                ag_ring(sb, d, r - 1).wait_recv()
                if r < HOPS[d]:
                    ag_ring(sb, d, r).start()
                ag_partner(sb, z - sign(sb, d) * r).start()

    def ag_wait(sb):
        def body(i, _):
            ag_partner(sb, i).wait_recv()
            return 0
        lax.fori_loop(0, nz, body, 0)

    def n_loads(b):
        sb, j = b // per_sb, lax.rem(b, per_sb)
        return [pltpu.make_async_copy(n_all.at[j * TILES + a, :, lanes_of(sb)],
                                      nblk.at[lax.rem(b, 4), :, pl.ds(a * LANE, LANE)],
                                      nl_sem.at[lax.rem(b, 4), a]) for a in range(TILES)]

    def dn_moves(b):
        sb, j, sl = b // per_sb, lax.rem(b, per_sb), lax.rem(b, 2)
        out = []
        for h in range(TILES // CORES):
            chip = j * (TILES // CORES) + h
            here = pl.ds(pl.multiple_of((h * CORES + core) * LANE, LANE), LANE)
            there = pl.ds(pl.multiple_of((h * CORES + 1 - core) * LANE, LANE), LANE)
            out.append((pltpu.make_async_copy(dnb.at[sl, :, here], dnp.at[sb, chip], dnp_sem.at[sl, h]),
                        remote(dnb.at[sl, :, there], prx.at[sb, chip], pair_send.at[sl, h],
                               pair_recv.at[sb, chip], partner)))
        return out

    def tile_loads(sb, chip, k):
        chip = lax.rem(chip + 2 * nz, nz)
        return [pltpu.make_async_copy(dnp.at[sb, chip], ownv.at[k, 0], ov_sem.at[k, 0]),
                pltpu.make_async_copy(prx.at[sb, chip], ownv.at[k, 1], ov_sem.at[k, 1])]

    def rx_slot(sb, d, r):
        return rx.at[lax.rem(sb, 2), d * HOPS[0] + r]

    def ring_copy(sb, d, r):
        return remote(sendb.at[d], rx_slot(sb, d, r), ring_send.at[d],
                      ring_recv.at[lax.rem(sb, 2), d * HOPS[0] + r], at(dev(z + sign(sb, d))))

    def ring_target(sb, d, r):
        return z + sign(sb, d) * (HOPS[d] - r)

    def st_pair(b):
        sl = lax.rem(b, 4)
        return remote(own_s.at[sl, 1 - core], x1.at[sl], st_send.at[sl, 0], st_recv.at[sl, 0], partner)

    def st_chip(b, k):
        sl = lax.rem(b, 4)
        return remote(x2.at[sl, z], x2.at[sl, z], st_send.at[sl, k], st_recv.at[sl, nz - k], at(dev(z + k)))

    def st_back(b):
        sl = lax.rem(b, 4)
        return remote(Sb.at[sl, core], Sb.at[sl, core], st_send.at[sl, nz], st_recv.at[sl, nz], partner)

    def lab_copy(k):
        return remote(lab_own, lab_all.at[me], lab_send.at[k - 1], lab_recv.at[n_pp - 1 - k],
                      at(lax.rem(me + k, n_pp)))

    own_copy = pltpu.make_async_copy(n_own, n_all.at[me], io_sem.at[0])
    own_copy.start()
    barrier = pltpu.get_barrier_semaphore()
    for k in range(1, n_pp):
        pl.semaphore_signal(barrier, inc=1, device_id=at(lax.rem(me + k, n_pp)), device_id_type=MESH)
    pl.semaphore_wait(barrier, n_pp - 1)
    ag_first(0)
    for k in range(1, n_pp):
        lab_copy(k).start()
    lab_all[me] = lab_own[...]
    dW[...] = jnp.zeros_like(dW)
    for r in range(1, HOPS[0] + 1):
        ag_next(0, r)
        if r == HOPS[0] - 1 and nsb > 1:
            ag_first(1)
    own_copy.wait()
    ag_wait(0)
    for c in n_loads(0):
        c.start()

    base = me * V

    def forward(b):
        for c in n_loads(b):
            c.wait()
        zl = jnp.dot(W[...], nblk[lax.rem(b, 4)], preferred_element_type=F32)
        t = jnp.tanh(zl * (1.0 / SOFT_CAP))
        U[lax.rem(b, 3)] = t
        s = jnp.sum(jnp.exp2(t * EXP2_SCALE).reshape(V // 8, 8, TB), axis=0)
        s = jnp.sum(s, axis=0, keepdims=True)
        for h in range(CORES):
            own_s[lax.rem(b, 4), h] = s[:, h * HALF:(h + 1) * HALF]
        st_pair(b).start()

    def backward(b):
        sl4 = lax.rem(b, 4)
        st_back(b).wait_recv()
        sb, j = b // per_sb, lax.rem(b, per_sb)
        for h in range(CORES):
            s = Sb[sl4, h]
            s_out[b, :, h * HALF:(h + 1) * HALF] = s
            svec[:, h * HALF:(h + 1) * HALF] = 1.0 / (s * total)
        for a in range(TILES):
            labm[:, a * LANE:(a + 1) * LANE] = lab_all[j * TILES + a, :, lanes_of(sb)] - base
        t = U[lax.rem(b, 3)]
        p = jnp.exp2(t * EXP2_SCALE) * svec[...]
        hit = lax.broadcasted_iota(jnp.int32, (V, TB), 0) == labm[...]
        tl = jnp.sum(jnp.where(hit, t, 0.0).reshape(V // 8, 8, TB), axis=0)
        g = p - jnp.where(hit, 1.0 / total, 0.0)
        dz = (g * (1.0 - t * t)).astype(BF16)
        sl = lax.rem(b, 2)
        dnb[sl, pl.ds(0, D), :] = jnp.dot(WT[...], dz, preferred_element_type=F32)
        dnb[sl, pl.ds(D, PAD_ROWS), :] = tl
        dW[...] += lax.dot_general(nblk[sl4], dz, (((1,), (1,)), ((), ())), preferred_element_type=F32)
        for keep, give in dn_moves(b):
            keep.start()
            give.start()
        st_pair(b).wait_send()
        for k in range(1, nz):
            st_chip(b, k).wait_send()
        st_back(b).wait_send()

    RS0 = per_sb + 3

    def step(s, _):
        @pl.when((s >= 1) & (s - 1 < nb))
        def _():
            b = s - 1
            sl = lax.rem(b, 4)
            st_pair(b).wait_recv()
            x2[sl, z] = own_s[sl, core] + x1[sl]
            for k in range(1, nz):
                st_chip(b, k).start()

        @pl.when((s >= 2) & (s - 2 < nb))
        def _():
            b = s - 2
            sl = lax.rem(b, 4)
            for k in range(1, nz):
                st_chip(b, k).wait_recv()
            acc = x2[sl, 0]
            for k in range(1, nz):
                acc = acc + x2[sl, k]
            Sb[sl, core] = acc
            st_back(b).start()

        for r in range(HOPS[0], 0, -1):
            sb = s + 2 - r

            @pl.when((sb >= 1) & (sb < nsb))
            def _():
                ag_next(sb, r)

        @pl.when(s + 2 < nsb)
        def _():
            ag_first(s + 2)

        @pl.when((lax.rem(s + 1, per_sb) == 0) & (s + 1 < nb))
        def _():
            ag_wait((s + 1) // per_sb)

        @pl.when(s + 1 < nb)
        def _():
            for c in n_loads(s + 1):
                c.start()

        @pl.when((s >= 4) & (s - 4 < nb))
        def _():
            for keep, give in dn_moves(s - 4):
                keep.wait()
                give.wait_send()

        q = s - RS0
        rsb, r = q // per_sb, lax.rem(q, per_sb)

        @pl.when((q >= 0) & (rsb < nsb) & (r == 0))
        def _():
            def body(i, _):
                remote(dnb.at[0, :, pl.ds(0, LANE)], prx.at[rsb, i], pair_send.at[0, 0], pair_recv.at[rsb, i],
                       partner).wait_recv()
                return 0
            lax.fori_loop(0, nz, body, 0)

        @pl.when((q >= 0) & (rsb < nsb))
        def _():
            for d in (0, 1):
                @pl.when(r < HOPS[d])
                def _():
                    for c in tile_loads(rsb, ring_target(rsb, d, r), d):
                        c.start()

        last = (q >= per_sb) & (r == 0)

        @pl.when(last)
        def _():
            for c in tile_loads(rsb - 1, z, 2):
                c.start()

        @pl.when(s < nb)
        def _():
            forward(s)

        @pl.when((q >= 1) & (q - 1 < nsb * per_sb))
        def _():
            for d in (0, 1):
                @pl.when(lax.rem(q - 1, per_sb) < HOPS[d])
                def _():
                    ring_copy((q - 1) // per_sb, d, lax.rem(q - 1, per_sb)).wait_send()

        @pl.when(last)
        def _():
            for c in tile_loads(rsb - 1, z, 2):
                c.wait()
            for d in (0, 1):
                ring_copy(rsb - 1, d, HOPS[d] - 1).wait_recv()

            @pl.when(q >= 2 * per_sb)
            def _():
                pltpu.make_async_copy(outv, dn_out.at[:, lanes_of(rsb - 2)], io_sem.at[1]).wait()
            acc = ownv[2, 0] + ownv[2, 1]
            for d in (0, 1):
                acc = acc + rx[lax.rem(rsb - 1, 2), d * HOPS[0] + HOPS[d] - 1]
            outv[...] = acc
            pltpu.make_async_copy(outv, dn_out.at[:, lanes_of(rsb - 1)], io_sem.at[1]).start()

        @pl.when((q >= 0) & (rsb < nsb))
        def _():
            for d in (0, 1):
                @pl.when(r < HOPS[d])
                def _():
                    for c in tile_loads(rsb, ring_target(rsb, d, r), d):
                        c.wait()

                    @pl.when(r == 0)
                    def _():
                        sendb[d] = ownv[d, 0] + ownv[d, 1]

                    @pl.when(r > 0)
                    def _():
                        ring_copy(rsb, d, r - 1).wait_recv()
                        sendb[d] = ownv[d, 0] + ownv[d, 1] + rx[lax.rem(rsb, 2), d * HOPS[0] + r - 1]
                    ring_copy(rsb, d, r).start()

        @pl.when(s == 2)
        def _():
            for k in range(1, n_pp):
                lab_copy(k).wait_recv()

        @pl.when((s >= 2) & (s - 2 < nb))
        def _():
            backward(s - 2)
        return 0
    lax.fori_loop(0, RS0 + nsb * per_sb + 1, step, 0)

    pltpu.make_async_copy(outv, dn_out.at[:, lanes_of(nsb - 1)], io_sem.at[1]).wait()
    w_store = pltpu.make_async_copy(dW, dW_out, io_sem.at[0])
    w_store.start()
    for k in range(1, n_pp):
        lab_copy(k).wait_send()

    def finish(sb, _):
        for d in (0, 1):
            for r in range(HOPS[d]):
                ag_ring(sb, d, r).wait_send()

        def body(i, _):
            ag_partner(sb, i).wait_send()
            return 0
        lax.fori_loop(0, nz, body, 0)
        return 0
    lax.fori_loop(0, nsb, finish, 0)
    w_store.wait()


def mega_call(n_own, lab_own, W, WT, *, n_pp, total, cid=1):
    D, T = n_own.shape
    V = W.shape[0]
    D8, nz, nsb = D + PAD_ROWS, n_pp // CORES, T // LANE
    nb = nsb * n_pp // TILES
    hbm, vmem = pl.BlockSpec(memory_space=pl.ANY), pl.BlockSpec(memory_space=pltpu.VMEM)
    dma, sd = pltpu.SemaphoreType.DMA, jax.ShapeDtypeStruct
    out = pl.pallas_call(
        functools.partial(kernel, n_pp, float(total)),
        out_shape=[sd((D8, T), F32), sd((D, V), F32), sd((nb, 1, TB), F32),
                   sd((n_pp, D, T), BF16), sd((nsb, nz, D8, LANE), F32), sd((nsb, nz, D8, LANE), F32)],
        in_specs=[vmem] * 4,
        out_specs=[hbm, hbm, vmem, hbm, hbm, hbm],
        scratch_shapes=[
            pltpu.VMEM((3, V, TB), F32), pltpu.VMEM((4, D, TB), BF16), pltpu.VMEM((D, V), F32),
            pltpu.VMEM((2, D8, TB), F32), pltpu.VMEM((1, TB), F32), pltpu.VMEM((1, TB), jnp.int32),
            pltpu.VMEM((n_pp, 1, T), jnp.int32), pltpu.VMEM((4, CORES, 1, HALF), F32), pltpu.VMEM((4, 1, HALF), F32),
            pltpu.VMEM((4, nz, 1, HALF), F32), pltpu.VMEM((4, CORES, 1, HALF), F32),
            pltpu.VMEM((2, sum(HOPS), D8, LANE), F32), pltpu.VMEM((3, 2, D8, LANE), F32),
            pltpu.VMEM((2, D8, LANE), F32), pltpu.VMEM((D8, LANE), F32),
            dma((nsb, 2, HOPS[0])), dma((nsb, 2, HOPS[0])), dma((nsb, nz)), dma((nsb, nz)),
            dma((nsb, nz)), dma((2, 2)), dma((2, 2)), dma((2, sum(HOPS))), dma((2,)),
            dma((4, nz + 1)), dma((4, nz + 1)), dma((n_pp - 1,)), dma((n_pp - 1,)), dma((4, TILES)), dma((3, 2)), dma((2,)),
        ],
        compiler_params=pltpu.CompilerParams(vmem_limit_bytes=63 * 1024 * 1024, collective_id=cid, has_side_effects=True),
        cost_estimate=pl.CostEstimate(flops=6 * n_pp * T * D * V, bytes_accessed=n_pp * T * D * 20, transcendentals=0),
        name="head")(n_own, lab_own, W, WT)
    return out[:3]


def sum_kernel(n_pp, x_ref, o_ref, rbuf, send_sem, recv_sem):
    me = lax.axis_index("pp")

    def peer(k):
        return {"pp": lax.rem(me + k, n_pp)}

    barrier = pltpu.get_barrier_semaphore()
    for k in range(1, n_pp):
        pl.semaphore_signal(barrier, inc=1, device_id=peer(k), device_id_type=MESH)
    pl.semaphore_wait(barrier, n_pp - 1)
    copies = [pltpu.make_async_remote_copy(
        src_ref=x_ref, dst_ref=rbuf.at[me], send_sem=send_sem.at[k - 1], recv_sem=recv_sem.at[n_pp - 1 - k],
        device_id=peer(k), device_id_type=MESH) for k in range(1, n_pp)]
    for c in copies:
        c.start()
    for c in copies:
        c.wait_recv()
    acc = jnp.zeros_like(o_ref)
    for k in range(n_pp):
        acc = acc + jnp.where(k == me, x_ref[...], rbuf[k])
    o_ref[...] = acc
    for c in copies:
        c.wait_send()


def small_sum(x, n_pp, cid):
    vmem = pl.BlockSpec(memory_space=pltpu.VMEM)
    return pl.pallas_call(
        functools.partial(sum_kernel, n_pp), out_shape=jax.ShapeDtypeStruct(x.shape, F32),
        in_specs=[vmem], out_specs=vmem,
        scratch_shapes=[pltpu.VMEM((n_pp,) + x.shape, F32), pltpu.SemaphoreType.DMA((n_pp - 1,)),
                        pltpu.SemaphoreType.DMA((n_pp - 1,))],
        compiler_params=pltpu.CompilerParams(collective_id=cid, has_side_effects=True), name="small_sum")(x)


def norm_cols(cols, gain):
    mean_sq = jnp.mean(cols * cols, axis=1, keepdims=True)
    return cols * lax.rsqrt(mean_sq + EPS) * (1.0 + gain)[None, :, None]


def solution(mesh):
    n_pp = mesh.shape["pp"]

    def local_fn(hidden, labels, gamma, table):
        mb, seq, D = hidden.shape
        V = table.shape[0]
        T = mb * seq
        total = T * n_pp
        me = lax.axis_index("pp")
        cols = jnp.swapaxes(hidden, 1, 2).astype(F32)
        normed, norm_vjp = jax.vjp(norm_cols, cols, gamma)
        normed = jnp.concatenate(list(normed.astype(BF16)), axis=1)
        dn, dW, s = mega_call(normed, labels.reshape(1, T), table, table.T, n_pp=n_pp, total=total)
        s = lax.dynamic_index_in_dim(s.reshape(T // LANE, n_pp, LANE), me, 1, keepdims=False).reshape(T)
        loss = jnp.log(s) - SOFT_CAP * jnp.sum(dn[D:], axis=0)
        d_cols, d_gain = norm_vjp(dn[:D].reshape(D, mb, seq).swapaxes(0, 1))
        flat = jnp.concatenate([d_gain, jnp.sum(loss)[None]])
        rows = -(-flat.shape[0] // 1024) * 8
        flat = jnp.pad(flat, (0, rows * 128 - flat.shape[0])).reshape(rows, 128)
        flat = small_sum(flat, n_pp, 2).reshape(-1)
        return (loss.reshape(mb, seq), jnp.swapaxes(d_cols, 1, 2).astype(BF16), flat[D:D + 1] / total,
                dW.T, flat[:D])

    token_spec = P(("dp", "pp"))
    return jax.shard_map(local_fn, mesh=mesh,
                         in_specs=(token_spec, token_spec, P(), P("pp")),
                         out_specs=(token_spec, token_spec, P("dp"), token_spec, P("dp")),
                         check_vma=False)
```

```python
import functools
import math

import jax
import jax.numpy as jnp
from jax import lax
from jax.experimental import pallas as pl
from jax.experimental.pallas import tpu as pltpu
from jax.sharding import PartitionSpec as P

F32, BF16 = jnp.float32, jnp.bfloat16
SOFT_CAP = 30.0
EPS = 1e-6
EXP2_SCALE = SOFT_CAP * math.log2(math.e)
MESH = pl.DeviceIdType.MESH
CORES = 2
LANE = 128
TILES = 4
TB = LANE * TILES
HALF = TB // CORES
PAD_ROWS = 8
PIECES = 4
WROWS = 256
HOPS = (4, 3)


def kernel(n_pp, total, hid, lab_own, gamma, WT,
           dh, dW, loss_out, ex_out, n_all, dnp, prx,
           n_own, W, gain, rinv, dgacc, lacc, s_out, ex_own, ex_rx,
           U, nblk, dnb, svec, labm, lab_all, own_s, x1, x2, Sb, rx, ownv, sendb,
           ag_recv, ag_send, pag_recv, pag_send, pair_recv, pair_send, dnp_sem, ring_recv, ring_send,
           st_recv, st_send, lab_recv, lab_send, nl_sem, ov_sem, io_sem, tail_recv, tail_send, tl_sem, ex_recv, ex_send,
           first_recv, first_send, firstp_recv, firstp_send):
    D, T = n_own.shape
    V = W.shape[0]
    seq = hid.shape[2]
    per_mb = seq // LANE
    wrows = min(WROWS, V)
    D8 = D + PAD_ROWS
    nz = n_pp // CORES
    nsb = T // LANE
    per_sb = n_pp // TILES
    nb = nsb * per_sb
    me = lax.axis_index("pp")
    z, core = me // CORES, lax.rem(me, CORES)

    def dev(chip, c=core):
        return lax.rem(chip + 2 * nz, nz) * CORES + c

    def at(index):
        return {"pp": index}

    partner = at(z * CORES + 1 - core)

    def lanes_of(sb):
        return pl.ds(pl.multiple_of(sb * LANE, LANE), LANE)

    def remote(src, dst, ssem, rsem, where):
        return pltpu.make_async_remote_copy(src_ref=src, dst_ref=dst, send_sem=ssem, recv_sem=rsem,
                                            device_id=where, device_id_type=MESH)

    def mb_lanes(sb):
        return pl.ds(pl.multiple_of(lax.rem(sb, per_mb) * LANE, LANE), LANE)

    def sign(sb, d):
        g = 1 - 2 * lax.rem(sb, 2)
        return g if d == 0 else -g

    def ag_ring(sb, d, r):
        g = sign(sb, d)
        if r == 0:
            src = n_own.at[:, lanes_of(sb)]
        else:
            src = n_all.at[dev(z - g * r), :, lanes_of(sb)]
        return remote(src, n_all.at[dev(z - g * r), :, lanes_of(sb)], ag_send.at[sb, d, r], ag_recv.at[sb, d, r],
                      at(dev(z + g)))

    def ag_partner(sb, chip, own=False):
        i = lax.rem(chip + 2 * nz, nz)
        src = n_own.at[:, lanes_of(sb)] if own else n_all.at[dev(chip), :, lanes_of(sb)]
        return remote(src, n_all.at[dev(chip), :, lanes_of(sb)], pag_send.at[sb, i], pag_recv.at[sb, i], partner)

    rows0 = D // PIECES

    def first_ring(d, r, p):
        g = sign(0, d)
        rows = pl.ds(p * rows0, rows0)
        src = n_own.at[rows, pl.ds(0, LANE)] if r == 0 else n_all.at[dev(z - g * r), rows, pl.ds(0, LANE)]
        return remote(src, n_all.at[dev(z - g * r), rows, pl.ds(0, LANE)], first_send.at[d, r, p],
                      first_recv.at[d, r, p], at(dev(z + g)))

    def first_partner(d, r, p):
        g = sign(0, d)
        rows = pl.ds(p * rows0, rows0)
        src = n_own.at[rows, pl.ds(0, LANE)] if r == 0 else n_all.at[dev(z - g * r), rows, pl.ds(0, LANE)]
        return remote(src, n_all.at[dev(z - g * r), rows, pl.ds(0, LANE)], firstp_send.at[d, r, p],
                      firstp_recv.at[d, r, p], partner)

    FIRSTP = [(d, r) for r in range(HOPS[0] + 1) for d in (0, 1) if r <= HOPS[d] and (r, d) != (0, 1)]

    def ag_first(sb):
        for d in (0, 1):
            ag_ring(sb, d, 0).start()
        ag_partner(sb, z, own=True).start()

    def ag_next(sb, r):
        for d in (0, 1):
            if r <= HOPS[d]:
                ag_ring(sb, d, r - 1).wait_recv()
                if r < HOPS[d]:
                    ag_ring(sb, d, r).start()
                ag_partner(sb, z - sign(sb, d) * r).start()

    def ag_wait(sb):
        def body(i, _):
            ag_partner(sb, i).wait_recv()
            return 0
        lax.fori_loop(0, nz, body, 0)

    def n_loads(b):
        sb, j = b // per_sb, lax.rem(b, per_sb)
        return [pltpu.make_async_copy(n_all.at[j * TILES + a, :, lanes_of(sb)],
                                      nblk.at[lax.rem(b, 4), :, pl.ds(a * LANE, LANE)],
                                      nl_sem.at[lax.rem(b, 4), a]) for a in range(TILES)]

    def dn_moves(b):
        sb, j, sl = b // per_sb, lax.rem(b, per_sb), lax.rem(b, 2)
        out = []
        for h in range(TILES // CORES):
            chip = j * (TILES // CORES) + h
            here = pl.ds(pl.multiple_of((h * CORES + core) * LANE, LANE), LANE)
            there = pl.ds(pl.multiple_of((h * CORES + 1 - core) * LANE, LANE), LANE)
            out.append((pltpu.make_async_copy(dnb.at[sl, :, here], dnp.at[sb, chip], dnp_sem.at[sl, h]),
                        remote(dnb.at[sl, :, there], prx.at[sb, chip], pair_send.at[sl, h],
                               pair_recv.at[sb, chip], partner)))
        return out

    def tile_loads(sb, chip, k):
        chip = lax.rem(chip + 2 * nz, nz)
        return [pltpu.make_async_copy(dnp.at[sb, chip], ownv.at[k, 0], ov_sem.at[k, 0]),
                pltpu.make_async_copy(prx.at[sb, chip], ownv.at[k, 1], ov_sem.at[k, 1])]

    def rx_slot(sb, d, r):
        return rx.at[lax.rem(sb, 2), d * HOPS[0] + r]

    cut = D8 // 16 * 8
    part = (pl.ds(0, cut), pl.ds(cut, D8 - cut))

    def ring_copy(sb, d, r, h):
        return remote(sendb.at[d, part[h]], rx_slot(sb, d, r).at[part[h]], ring_send.at[d, h],
                      ring_recv.at[lax.rem(sb, 2), d * HOPS[0] + r, h], at(dev(z + sign(sb, d))))

    def ring_step(q, h):
        sb, r = q // per_sb, lax.rem(q, per_sb)
        for d in (0, 1):
            @pl.when((q >= 1) & (q - 1 < n_rs * per_sb) & (lax.rem(q - 1, per_sb) < HOPS[d]))
            def _():
                ring_copy((q - 1) // per_sb, d, lax.rem(q - 1, per_sb), h).wait_send()

            @pl.when((q >= 0) & (sb < n_rs) & (r < HOPS[d]))
            def _():
                if h == 0:
                    for c in tile_loads(sb, ring_target(sb, d, r), d):
                        c.wait()

                @pl.when(r == 0)
                def _():
                    sendb[d, part[h], :] = ownv[d, 0, part[h], :] + ownv[d, 1, part[h], :]

                @pl.when(r > 0)
                def _():
                    ring_copy(sb, d, r - 1, h).wait_recv()
                    sendb[d, part[h], :] = (ownv[d, 0, part[h], :] + ownv[d, 1, part[h], :]
                                            + rx[lax.rem(sb, 2), d * HOPS[0] + r - 1, part[h], :])
                ring_copy(sb, d, r, h).start()

    def own_tile(sb):
        for c in tile_loads(sb, z, 2):
            c.wait()
        for d in (0, 1):
            for h in (0, 1):
                ring_copy(sb, d, HOPS[d] - 1, h).wait_recv()
        acc = ownv[2, 0] + ownv[2, 1]
        for d in (0, 1):
            acc = acc + rx[lax.rem(sb, 2), d * HOPS[0] + HOPS[d] - 1]
        finish_tile(sb, acc)

    def ring_target(sb, d, r):
        return z + sign(sb, d) * (HOPS[d] - r)

    def st_pair(b):
        sl = lax.rem(b, 4)
        return remote(own_s.at[sl, 1 - core], x1.at[sl], st_send.at[sl, 0], st_recv.at[sl, 0], partner)

    def st_chip(b, k):
        sl = lax.rem(b, 4)
        return remote(x2.at[sl, z], x2.at[sl, z], st_send.at[sl, k], st_recv.at[sl, nz - k], at(dev(z + k)))

    def st_back(b):
        sl = lax.rem(b, 4)
        return remote(Sb.at[sl, core], Sb.at[sl, core], st_send.at[sl, nz], st_recv.at[sl, nz], partner)

    def lab_copy(k):
        return remote(lab_own, lab_all.at[me], lab_send.at[k - 1], lab_recv.at[n_pp - 1 - k],
                      at(lax.rem(me + k, n_pp)))

    def hid_tile(sb):
        return hid[sb // per_mb, :, mb_lanes(sb)].astype(F32)

    def norm_tile(sb):
        h = hid_tile(sb)
        r = lax.rsqrt(jnp.mean(h * h, axis=0, keepdims=True) + EPS)
        rinv[sb] = r
        n_own[:, lanes_of(sb)] = (h * r * gain[...]).astype(BF16)

    def turn_table(c):
        rows = pl.ds(pl.multiple_of(c * wrows, wrows), wrows)
        W[rows, :] = WT[:, rows].T

    gain[...] = jnp.broadcast_to(1.0 + gamma[...], (LANE, D)).T
    norm_tile(0)
    barrier = pltpu.get_barrier_semaphore()
    for k in range(1, n_pp):
        pl.semaphore_signal(barrier, inc=1, device_id=at(lax.rem(me + k, n_pp)), device_id_type=MESH)
    pl.semaphore_wait(barrier, n_pp - 1)
    for p in range(PIECES):
        for d in (0, 1):
            first_ring(d, 0, p).start()
        first_partner(0, 0, p).start()
    for k in range(1, n_pp):
        lab_copy(k).start()
    lab_all[me] = lab_own[...]

    def rest(sb, _):
        norm_tile(sb)
        return 0
    lax.fori_loop(1, nsb, rest, 0)
    own_copy = pltpu.make_async_copy(n_own, n_all.at[me], io_sem.at[0])
    own_copy.start()
    dW[...] = jnp.zeros_like(dW)
    dgacc[...] = jnp.zeros_like(dgacc)
    lacc[...] = jnp.zeros_like(lacc)
    n_turn = V // wrows
    for r in range(1, HOPS[0] + 1):
        def turn(c, _):
            turn_table(c)
            return 0
        lax.fori_loop(n_turn * (r - 1) // HOPS[0], n_turn * r // HOPS[0], turn, 0)
        for p in range(PIECES):
            for d in (0, 1):
                if r <= HOPS[d]:
                    first_ring(d, r - 1, p).wait_recv()
                    if r < HOPS[d]:
                        first_ring(d, r, p).start()
                    first_partner(d, r, p).start()
        if r == HOPS[0] - 1 and nsb > 1:
            ag_first(1)
    own_copy.wait()
    for d, r in FIRSTP:
        for p in range(PIECES):
            first_partner(d, r, p).wait_recv()
    for c in n_loads(0):
        c.start()

    base = me * V

    def forward(b):
        for c in n_loads(b):
            c.wait()
        zl = jnp.dot(W[...], nblk[lax.rem(b, 4)], preferred_element_type=F32)
        t = jnp.tanh(zl * (1.0 / SOFT_CAP))
        U[lax.rem(b, 3), pl.ds(0, V), :] = t
        s = jnp.sum(jnp.exp2(t * EXP2_SCALE).reshape(V // 8, 8, TB), axis=0)
        s = jnp.sum(s, axis=0, keepdims=True)
        for h in range(CORES):
            own_s[lax.rem(b, 4), h] = s[:, h * HALF:(h + 1) * HALF]
        st_pair(b).start()

    def backward(b):
        sl4 = lax.rem(b, 4)
        st_back(b).wait_recv()
        sb, j = b // per_sb, lax.rem(b, per_sb)
        for h in range(CORES):
            s = Sb[sl4, h]
            s_out[b, :, h * HALF:(h + 1) * HALF] = s
            svec[:, h * HALF:(h + 1) * HALF] = 1.0 / (s * total)
        for a in range(TILES):
            rows = lab_all[j * TILES + a, :, mb_lanes(sb)]
            row = rows[0:1]
            for m in range(1, rows.shape[0]):
                row = jnp.where(sb // per_mb == m, rows[m:m + 1], row)
            labm[:, a * LANE:(a + 1) * LANE] = row - base
        t = U[lax.rem(b, 3), pl.ds(0, V), :]
        p = jnp.exp2(t * EXP2_SCALE) * svec[...]
        hit = lax.broadcasted_iota(jnp.int32, (V, TB), 0) == labm[...]
        tl = jnp.sum(jnp.where(hit, t, 0.0).reshape(V // 8, 8, TB), axis=0)
        g = p - jnp.where(hit, 1.0 / total, 0.0)
        dz = (g * (1.0 - t * t)).astype(BF16)
        sl = lax.rem(b, 2)
        dnb[sl, pl.ds(0, D), :] = jnp.dot(WT[...], dz, preferred_element_type=F32)
        dnb[sl, pl.ds(D, PAD_ROWS), :] = tl
        dW[...] += lax.dot_general(nblk[sl4], dz, (((1,), (1,)), ((), ())), preferred_element_type=F32)
        for keep, give in dn_moves(b):
            keep.start()
            give.start()
        st_pair(b).wait_send()
        for k in range(1, nz):
            st_chip(b, k).wait_send()
        st_back(b).wait_send()

    def finish_tile(sb, acc):
        dn = acc[0:D]
        h = hid_tile(sb)
        r = rinv[sb]
        xhat = h * r
        dgacc[...] += dn * xhat
        dx = dn * gain[...]
        m = jnp.mean(dx * xhat, axis=0, keepdims=True)
        dh[sb // per_mb, :, mb_lanes(sb)] = (
            r * (dx - xhat * m)).astype(BF16)
        own_s = s_out[sb * per_sb + me // TILES, :, pl.ds(pl.multiple_of(lax.rem(me, TILES) * LANE, LANE), LANE)]
        loss = jnp.log(own_s) - SOFT_CAP * jnp.sum(acc[D:D8], axis=0, keepdims=True)
        for m in range(hid.shape[0]):
            @pl.when(sb // per_mb == m)
            def _():
                loss_out[m:m + 1, mb_lanes(sb)] = loss
        lacc[...] += loss

    RS0 = per_sb + 3
    n_rs = nsb - 1

    def step(s, _):
        @pl.when((s >= 1) & (s - 1 < nb))
        def _():
            b = s - 1
            sl = lax.rem(b, 4)
            st_pair(b).wait_recv()
            x2[sl, z] = own_s[sl, core] + x1[sl]
            for k in range(1, nz):
                st_chip(b, k).start()

        @pl.when((s >= 2) & (s - 2 < nb))
        def _():
            b = s - 2
            sl = lax.rem(b, 4)
            for k in range(1, nz):
                st_chip(b, k).wait_recv()
            acc = x2[sl, 0]
            for k in range(1, nz):
                acc = acc + x2[sl, k]
            Sb[sl, core] = acc
            st_back(b).start()

        for r in range(HOPS[0], -1, -1):
            u = s - r
            sb = jnp.where(u <= 1, u + 2, jnp.where(u <= 5, u + 1, 7 + (u - 12) // 4))
            now = ((u >= -1) & (u <= 1)) | ((u >= 3) & (u <= 5)) | ((u >= 12) & (lax.rem(u, 4) == 0))

            @pl.when(now & (sb >= 1) & (sb < nsb))
            def _():
                if r == 0:
                    ag_first(sb)
                else:
                    ag_next(sb, r)

        @pl.when((lax.rem(s + 1, per_sb) == 0) & (s + 1 < nb))
        def _():
            ag_wait((s + 1) // per_sb)

        @pl.when(s + 1 < nb)
        def _():
            for c in n_loads(s + 1):
                c.start()

        @pl.when((s >= 4) & (s - 4 < nb))
        def _():
            for keep, give in dn_moves(s - 4):
                keep.wait()
                give.wait_send()

        q = s - RS0
        rsb, r = q // per_sb, lax.rem(q, per_sb)

        @pl.when((q >= 0) & (rsb < n_rs) & (r == 0))
        def _():
            def body(i, _):
                remote(dnb.at[0, :, pl.ds(0, LANE)], prx.at[rsb, i], pair_send.at[0, 0], pair_recv.at[rsb, i],
                       partner).wait_recv()
                return 0
            lax.fori_loop(0, nz, body, 0)

        @pl.when((q >= 0) & (rsb < n_rs))
        def _():
            for d in (0, 1):
                @pl.when(r < HOPS[d])
                def _():
                    for c in tile_loads(rsb, ring_target(rsb, d, r), d):
                        c.start()

        last = (q >= per_sb) & (r == 0) & (rsb <= n_rs)

        @pl.when(last)
        def _():
            for c in tile_loads(rsb - 1, z, 2):
                c.start()

        @pl.when(s < nb)
        def _():
            forward(s)

        ring_step(q, 0)

        @pl.when(s == 2)
        def _():
            for k in range(1, n_pp):
                lab_copy(k).wait_recv()

        @pl.when((s >= 2) & (s - 2 < nb))
        def _():
            backward(s - 2)

        ring_step(q, 1)

        @pl.when(last)
        def _():
            own_tile(rsb - 1)
        return 0
    n_steps = RS0 + n_rs * per_sb
    lax.fori_loop(0, n_steps, step, 0)

    sb = nsb - 1
    par = sb % 2
    for b in range(max(n_steps - 4, 0), nb):
        for keep, give in dn_moves(b):
            keep.wait()
            give.wait_send()

    def prx_wait(i, _):
        remote(dnb.at[0, :, pl.ds(0, LANE)], prx.at[sb, i], pair_send.at[0, 0], pair_recv.at[sb, i],
               partner).wait_recv()
        return 0
    lax.fori_loop(0, nz, prx_wait, 0)

    def slot(half, e):
        return U.at[half, pl.ds(e // 4 * D8, D8), pl.ds(e % 4 * LANE, LANE)]

    hops = [(d, r) for r in range(HOPS[0]) for d in (0, 1) if r < HOPS[d]]
    loads = []
    for e, chip in enumerate([ring_target(sb, d, r) for d, r in hops] + [z]):
        chip = lax.rem(chip + 2 * nz, nz)
        loads.append([pltpu.make_async_copy(dnp.at[sb, chip], slot(0, e), tl_sem.at[0, e]),
                      pltpu.make_async_copy(prx.at[sb, chip], slot(1, e), tl_sem.at[1, e])])
        for c in loads[-1]:
            c.start()
    cuts = [D8 // 8 * p // PIECES * 8 for p in range(PIECES + 1)]

    def piece(p):
        return pl.ds(cuts[p], cuts[p + 1] - cuts[p])

    def tail_copy(e, p):
        d, r = hops[e]
        return remote(slot(0, e).at[piece(p)], rx.at[par, d * HOPS[0] + r, piece(p)],
                      tail_send.at[e, p], tail_recv.at[d * HOPS[0] + r, p], at(dev(z + sign(sb, d))))

    def tail_arrived(d, r, p):
        remote(slot(0, 0).at[piece(p)], rx.at[par, d * HOPS[0] + r, piece(p)], tail_send.at[0, p],
               tail_recv.at[d * HOPS[0] + r, p], partner).wait_recv()

    if n_rs > 0:
        for c in tile_loads(n_rs - 1, z, 2):
            c.start()
    for e, (d, r) in enumerate(hops):
        if r == 1 and d == 0 and n_rs > 0:
            for h in (0, 1):
                ring_step(jnp.int32(n_rs * per_sb), h)
            own_tile(n_rs - 1)
        for c in loads[e]:
            c.wait()
        for p in range(PIECES):
            mine, other = slot(0, e).at[piece(p)], slot(1, e).at[piece(p)]
            if r > 0:
                tail_arrived(d, r - 1, p)
                mine[...] = mine[...] + other[...] + rx[par, d * HOPS[0] + r - 1, piece(p)]
            else:
                mine[...] = mine[...] + other[...]
            tail_copy(e, p).start()
    for c in loads[len(hops)]:
        c.wait()
    for d in (0, 1):
        for p in range(PIECES):
            tail_arrived(d, HOPS[d] - 1, p)
    finish_tile(sb, slot(0, len(hops))[...] + slot(1, len(hops))[...] + rx[par, HOPS[0] - 1]
                + rx[par, HOPS[0] + HOPS[1] - 1])

    ex_own[:, 0:D] = jnp.sum(dgacc[...].T, axis=0, keepdims=True)
    ex_own[:, pl.ds(ex_own.shape[1] - LANE, LANE)] = lacc[...]
    exs = [remote(ex_own, ex_rx.at[me], ex_send.at[k - 1], ex_recv.at[n_pp - 1 - k], at(lax.rem(me + k, n_pp)))
           for k in range(1, n_pp)]
    for c in exs:
        c.start()
    for c in exs:
        c.wait_recv()
    acc = jnp.zeros_like(ex_out)
    for k in range(n_pp):
        acc = acc + jnp.where(k == me, ex_own[...], ex_rx[k])
    ex_out[...] = acc
    for c in exs:
        c.wait_send()
    for e in range(len(hops)):
        for p in range(PIECES):
            tail_copy(e, p).wait_send()
    for k in range(1, n_pp):
        lab_copy(k).wait_send()

    for p in range(PIECES):
        for d in (0, 1):
            for r in range(HOPS[d]):
                first_ring(d, r, p).wait_send()
        for d, r in FIRSTP:
            first_partner(d, r, p).wait_send()

    def finish(sb, _):
        for d in (0, 1):
            for r in range(HOPS[d]):
                ag_ring(sb, d, r).wait_send()

        def body(i, _):
            ag_partner(sb, i).wait_send()
            return 0
        lax.fori_loop(0, nz, body, 0)
        return 0
    lax.fori_loop(1, nsb, finish, 0)


def mega_call(hid, lab_own, gamma, WT, *, n_pp, total, cid=1):
    mb, D, seq = hid.shape
    T = mb * seq
    V = WT.shape[1]
    D8, nz, nsb = D + PAD_ROWS, n_pp // CORES, T // LANE
    nb = nsb * n_pp // TILES
    EX = -(-D // LANE) * LANE + LANE
    hbm, vmem = pl.BlockSpec(memory_space=pl.ANY), pl.BlockSpec(memory_space=pltpu.VMEM)
    dma, sd = pltpu.SemaphoreType.DMA, jax.ShapeDtypeStruct
    out = pl.pallas_call(
        functools.partial(kernel, n_pp, float(total)),
        out_shape=[sd((mb, D, seq), BF16), sd((D, V), F32), sd((mb, seq), F32), sd((1, EX), F32),
                   sd((n_pp, D, T), BF16), sd((nsb, nz, D8, LANE), F32), sd((nsb, nz, D8, LANE), F32)],
        in_specs=[vmem] * 4,
        out_specs=[vmem, vmem, vmem, vmem, hbm, hbm, hbm],
        scratch_shapes=[
            pltpu.VMEM((D, T), BF16), pltpu.VMEM((V, D), BF16), pltpu.VMEM((D, LANE), F32), pltpu.VMEM((nsb, 1, LANE), F32),
            pltpu.VMEM((D, LANE), F32), pltpu.VMEM((1, LANE), F32), pltpu.VMEM((nb, 1, TB), F32),
            pltpu.VMEM((1, EX), F32), pltpu.VMEM((n_pp, 1, EX), F32),
            pltpu.VMEM((3, max(V, 2 * D8), TB), F32), pltpu.VMEM((4, D, TB), BF16),
            pltpu.VMEM((2, D8, TB), F32), pltpu.VMEM((1, TB), F32), pltpu.VMEM((1, TB), jnp.int32),
            pltpu.VMEM((n_pp, mb, seq), jnp.int32), pltpu.VMEM((4, CORES, 1, HALF), F32), pltpu.VMEM((4, 1, HALF), F32),
            pltpu.VMEM((4, nz, 1, HALF), F32), pltpu.VMEM((4, CORES, 1, HALF), F32),
            pltpu.VMEM((2, sum(HOPS), D8, LANE), F32), pltpu.VMEM((3, 2, D8, LANE), F32),
            pltpu.VMEM((2, D8, LANE), F32),
            dma((nsb, 2, HOPS[0])), dma((nsb, 2, HOPS[0])), dma((nsb, nz)), dma((nsb, nz)),
            dma((nsb, nz)), dma((2, 2)), dma((2, 2)), dma((2, sum(HOPS), 2)), dma((2, 2)),
            dma((4, nz + 1)), dma((4, nz + 1)), dma((n_pp - 1,)), dma((n_pp - 1,)), dma((4, TILES)), dma((3, 2)), dma((1,)),
            dma((sum(HOPS), PIECES)), dma((sum(HOPS), PIECES)), dma((2, sum(HOPS) + 1)),
            dma((n_pp - 1,)), dma((n_pp - 1,)),
            *[dma((2, HOPS[0] + 1, PIECES))] * 4,
        ],
        compiler_params=pltpu.CompilerParams(vmem_limit_bytes=63 * 1024 * 1024, collective_id=cid, has_side_effects=True),
        cost_estimate=pl.CostEstimate(flops=6 * n_pp * T * D * V, bytes_accessed=n_pp * T * D * 20, transcendentals=0),
        name="head")(hid, lab_own, gamma, WT)
    return out[:4]


def solution(mesh):
    n_pp = mesh.shape["pp"]

    def local_fn(hidden, labels, gamma, table):
        mb, seq, D = hidden.shape
        V = table.shape[0]
        T = mb * seq
        total = T * n_pp
        dh, dW, loss, sums = mega_call(jnp.swapaxes(hidden, 1, 2), labels, gamma.reshape(1, D), table.T,
                                       n_pp=n_pp, total=total)
        return (loss, jnp.swapaxes(dh, 1, 2), jnp.sum(sums[0, -LANE:])[None] / total, dW.T, sums[0, :D])

    token_spec = P(("dp", "pp"))
    return jax.shard_map(local_fn, mesh=mesh,
                         in_specs=(token_spec, token_spec, P(), P("pp")),
                         out_specs=(token_spec, token_spec, P("dp"), token_spec, P("dp")),
                         check_vma=False)
```

```python
import functools
import math

import jax
import jax.numpy as jnp
from jax import lax
from jax.experimental import pallas as pl
from jax.experimental.pallas import tpu as pltpu
from jax.sharding import PartitionSpec as P

F32, BF16 = jnp.float32, jnp.bfloat16
SOFT_CAP = 30.0
EPS = 1e-6
EXP2_SCALE = SOFT_CAP * math.log2(math.e)
MESH = pl.DeviceIdType.MESH
CORES = 2
LANE = 128
TILES = 4
TB = LANE * TILES
HALF = TB // CORES
PAD_ROWS = 8
PIECES = 4
WROWS = 256
FWD_PARTS = 24
HOPS = (4, 3)


def kernel(n_pp, total, hid, lab_own, gamma, WT,
           dh, dW_out, loss_out, ex_out, n_all, dnp, prx,
           n_own, W, gain, rinv, dgacc, lacc, s_out, ex_own, ex_rx,
           U, nblk, dW, dnb, svec, labm, tls, lab_all, own_s, x1, x2, Sb, rx, ownv, sendb,
           ag_recv, ag_send, pag_recv, pag_send, pair_recv, pair_send, dnp_sem, ring_recv, ring_send,
           st_recv, st_send, lab_recv, lab_send, nl_sem, ov_sem, io_sem, tail_recv, tail_send, tl_sem, ex_recv, ex_send,
           first_recv, first_send, firstp_recv, firstp_send):
    D, T = n_own.shape
    V = W.shape[0]
    seq = hid.shape[2]
    per_mb = seq // LANE
    wrows = min(WROWS, V)
    D8 = D + PAD_ROWS
    nz = n_pp // CORES
    nsb = T // LANE
    per_sb = n_pp // TILES
    nb = nsb * per_sb
    me = lax.axis_index("pp")
    z, core = me // CORES, lax.rem(me, CORES)

    def dev(chip, c=core):
        return lax.rem(chip + 2 * nz, nz) * CORES + c

    def at(index):
        return {"pp": index}

    partner = at(z * CORES + 1 - core)

    def lanes_of(sb):
        return pl.ds(pl.multiple_of(sb * LANE, LANE), LANE)

    def remote(src, dst, ssem, rsem, where):
        return pltpu.make_async_remote_copy(src_ref=src, dst_ref=dst, send_sem=ssem, recv_sem=rsem,
                                            device_id=where, device_id_type=MESH)

    def mb_lanes(sb):
        return pl.ds(pl.multiple_of(lax.rem(sb, per_mb) * LANE, LANE), LANE)

    def sign(sb, d):
        g = 1 - 2 * lax.rem(sb, 2)
        return g if d == 0 else -g

    def ag_ring(sb, d, r):
        g = sign(sb, d)
        if r == 0:
            src = n_own.at[:, lanes_of(sb)]
        else:
            src = n_all.at[dev(z - g * r), :, lanes_of(sb)]
        return remote(src, n_all.at[dev(z - g * r), :, lanes_of(sb)], ag_send.at[sb, d, r], ag_recv.at[sb, d, r],
                      at(dev(z + g)))

    def ag_partner(sb, chip, own=False):
        i = lax.rem(chip + 2 * nz, nz)
        src = n_own.at[:, lanes_of(sb)] if own else n_all.at[dev(chip), :, lanes_of(sb)]
        return remote(src, n_all.at[dev(chip), :, lanes_of(sb)], pag_send.at[sb, i], pag_recv.at[sb, i], partner)

    rows0 = D // PIECES

    def first_tile(chip, p):
        i = dev(chip)
        return nblk.at[i // TILES, pl.ds(p * rows0, rows0), pl.ds(pl.multiple_of(lax.rem(i, TILES) * LANE, LANE), LANE)]

    def first_ring(d, r, p):
        g = sign(0, d)
        ref = first_tile(z - g * r, p)
        return remote(ref, ref, first_send.at[d, r, p], first_recv.at[d, r, p], at(dev(z + g)))

    def first_partner(d, r, p):
        ref = first_tile(z - sign(0, d) * r, p)
        return remote(ref, ref, firstp_send.at[d, r, p], firstp_recv.at[d, r, p], partner)

    FIRSTP = [(d, r) for r in range(HOPS[0] + 1) for d in (0, 1) if r <= HOPS[d] and (r, d) != (0, 1)]

    def ag_first(sb):
        for d in (0, 1):
            ag_ring(sb, d, 0).start()
        ag_partner(sb, z, own=True).start()

    def ag_next(sb, r):
        for d in (0, 1):
            if r <= HOPS[d]:
                ag_ring(sb, d, r - 1).wait_recv()
                if r < HOPS[d]:
                    ag_ring(sb, d, r).start()
                ag_partner(sb, z - sign(sb, d) * r).start()

    def ag_wait(sb):
        def body(i, _):
            ag_partner(sb, i).wait_recv()
            return 0
        lax.fori_loop(0, nz, body, 0)

    def n_loads(b):
        sb, j = b // per_sb, lax.rem(b, per_sb)
        return [pltpu.make_async_copy(n_all.at[j * TILES + a, :, lanes_of(sb)],
                                      nblk.at[lax.rem(b, 4), :, pl.ds(a * LANE, LANE)],
                                      nl_sem.at[lax.rem(b, 4), a]) for a in range(TILES)]

    def dn_moves(b):
        sb, j, sl = b // per_sb, lax.rem(b, per_sb), lax.rem(b, 2)
        out = []
        for h in range(TILES // CORES):
            chip = j * (TILES // CORES) + h
            here = pl.ds(pl.multiple_of((h * CORES + core) * LANE, LANE), LANE)
            there = pl.ds(pl.multiple_of((h * CORES + 1 - core) * LANE, LANE), LANE)
            out.append((pltpu.make_async_copy(dnb.at[sl, :, here], dnp.at[sb, chip], dnp_sem.at[sl, h]),
                        remote(dnb.at[sl, :, there], prx.at[sb, chip], pair_send.at[sl, h],
                               pair_recv.at[sb, chip], partner)))
        return out

    def prx_arrived(sb, i):
        remote(dnb.at[0, :, pl.ds(0, LANE)], prx.at[sb, i], pair_send.at[0, 0], pair_recv.at[sb, i],
               partner).wait_recv()

    def tile_loads(sb, chip, k):
        chip = lax.rem(chip + 2 * nz, nz)
        return [pltpu.make_async_copy(dnp.at[sb, chip], ownv.at[k, 0], ov_sem.at[k, 0]),
                pltpu.make_async_copy(prx.at[sb, chip], ownv.at[k, 1], ov_sem.at[k, 1])]

    def rx_slot(sb, d, r):
        return rx.at[lax.rem(sb, 2), d * HOPS[0] + r]

    cut = D8 // 16 * 8
    part = (pl.ds(0, cut), pl.ds(cut, D8 - cut))

    def ring_copy(sb, d, r, h):
        return remote(sendb.at[d, part[h]], rx_slot(sb, d, r).at[part[h]], ring_send.at[d, h],
                      ring_recv.at[lax.rem(sb, 2), d * HOPS[0] + r, h], at(dev(z + sign(sb, d))))

    def ring_step(q, h):
        sb, r = q // per_sb, lax.rem(q, per_sb)
        for d in (0, 1):
            @pl.when((q >= 1) & (q - 1 < n_rs * per_sb) & (lax.rem(q - 1, per_sb) < HOPS[d]))
            def _():
                ring_copy((q - 1) // per_sb, d, lax.rem(q - 1, per_sb), h).wait_send()

            @pl.when((q >= 0) & (sb < n_rs) & (r < HOPS[d]))
            def _():
                if h == 0:
                    for c in tile_loads(sb, ring_target(sb, d, r), d):
                        c.wait()

                @pl.when(r == 0)
                def _():
                    sendb[d, part[h], :] = ownv[d, 0, part[h], :] + ownv[d, 1, part[h], :]

                @pl.when(r > 0)
                def _():
                    ring_copy(sb, d, r - 1, h).wait_recv()
                    sendb[d, part[h], :] = (ownv[d, 0, part[h], :] + ownv[d, 1, part[h], :]
                                            + rx[lax.rem(sb, 2), d * HOPS[0] + r - 1, part[h], :])
                ring_copy(sb, d, r, h).start()

    def own_tile(sb):
        for c in tile_loads(sb, z, 2):
            c.wait()
        for d in (0, 1):
            for h in (0, 1):
                ring_copy(sb, d, HOPS[d] - 1, h).wait_recv()
        acc = ownv[2, 0] + ownv[2, 1]
        for d in (0, 1):
            acc = acc + rx[lax.rem(sb, 2), d * HOPS[0] + HOPS[d] - 1]
        finish_tile(sb, acc)

    def ring_target(sb, d, r):
        return z + sign(sb, d) * (HOPS[d] - r)

    def st_pair(b):
        sl = lax.rem(b, 4)
        return remote(own_s.at[sl, 1 - core], x1.at[sl], st_send.at[sl, 0], st_recv.at[sl, 0], partner)

    def st_chip(b, k):
        sl = lax.rem(b, 4)
        return remote(x2.at[sl, z], x2.at[sl, z], st_send.at[sl, k], st_recv.at[sl, nz - k], at(dev(z + k)))

    def st_back(b):
        sl = lax.rem(b, 4)
        return remote(Sb.at[sl, core], Sb.at[sl, core], st_send.at[sl, nz], st_recv.at[sl, nz], partner)

    def lab_copy(k):
        return remote(lab_own, lab_all.at[me], lab_send.at[k - 1], lab_recv.at[n_pp - 1 - k],
                      at(lax.rem(me + k, n_pp)))

    def hid_tile(sb):
        return hid[sb // per_mb, :, mb_lanes(sb)].astype(F32)

    def norm_tile(sb):
        h = hid_tile(sb)
        r = lax.rsqrt(jnp.mean(h * h, axis=0, keepdims=True) + EPS)
        rinv[sb] = r
        n_own[:, lanes_of(sb)] = (h * r * gain[...]).astype(BF16)

    def turn_table(c):
        rows = pl.ds(pl.multiple_of(c * wrows, wrows), wrows)
        W[rows, :] = WT[:, rows].T

    gain[...] = jnp.broadcast_to(1.0 + gamma[...], (LANE, D)).T
    norm_tile(0)
    for p in range(PIECES):
        first_tile(z, p)[...] = n_own[p * rows0:(p + 1) * rows0, 0:LANE]
    barrier = pltpu.get_barrier_semaphore()
    for k in range(1, n_pp):
        pl.semaphore_signal(barrier, inc=1, device_id=at(lax.rem(me + k, n_pp)), device_id_type=MESH)
    pl.semaphore_wait(barrier, n_pp - 1)
    for p in range(PIECES):
        for d in (0, 1):
            first_ring(d, 0, p).start()
        first_partner(0, 0, p).start()
    for k in range(1, n_pp):
        lab_copy(k).start()
    lab_all[me] = lab_own[...]

    def rest(sb, _):
        norm_tile(sb)
        return 0
    lax.fori_loop(1, nsb, rest, 0)
    own_copy = pltpu.make_async_copy(n_own, n_all.at[me], io_sem.at[0])
    own_copy.start()
    dW[...] = jnp.zeros_like(dW)
    dgacc[...] = jnp.zeros_like(dgacc)
    lacc[...] = jnp.zeros_like(lacc)
    n_turn = V // wrows
    for r in range(1, HOPS[0] + 1):
        def turn(c, _):
            turn_table(c)
            return 0
        lax.fori_loop(n_turn * (r - 1) // HOPS[0], n_turn * r // HOPS[0], turn, 0)
        for p in range(PIECES):
            for d in (0, 1):
                if r <= HOPS[d]:
                    first_ring(d, r - 1, p).wait_recv()
                    if r < HOPS[d]:
                        first_ring(d, r, p).start()
                    first_partner(d, r, p).start()
        if r == HOPS[0] - 1 and nsb > 1:
            ag_first(1)
    if nsb > 2:
        ag_first(2)
    own_copy.wait()
    for d, r in FIRSTP:
        for p in range(PIECES):
            first_partner(d, r, p).wait_recv()
    for k in range(1, n_pp):
        lab_copy(k).wait_recv()

    base = me * V

    def forward(b):
        @pl.when(b >= per_sb)
        def _():
            for c in n_loads(b):
                c.wait()
        sl3 = lax.rem(b, 3)
        sb, j = b // per_sb, lax.rem(b, per_sb)
        for a in range(TILES):
            rows = lab_all[j * TILES + a, :, mb_lanes(sb)]
            row = rows[0:1]
            for m in range(1, rows.shape[0]):
                row = jnp.where(sb // per_mb == m, rows[m:m + 1], row)
            labm[sl3, :, a * LANE:(a + 1) * LANE] = row - base
        s = jnp.zeros((8, TB), F32)
        tl = jnp.zeros((8, TB), F32)
        n = V // FWD_PARTS
        for c in range(FWD_PARTS):
            zl = jnp.dot(W[c * n:(c + 1) * n, :], nblk[lax.rem(b, 4)], preferred_element_type=F32)
            t = jnp.tanh(zl * (1.0 / SOFT_CAP))
            e = jnp.exp2(t * EXP2_SCALE)
            U[sl3, c * n:(c + 1) * n, :] = e * (1.0 - t * t)
            hit = lax.broadcasted_iota(jnp.int32, (n, TB), 0) == labm[sl3] - c * n
            s = s + jnp.sum(e.reshape(n // 8, 8, TB), axis=0)
            tl = tl + jnp.sum(jnp.where(hit, t, 0.0).reshape(n // 8, 8, TB), axis=0)
        tls[sl3] = tl
        s = jnp.sum(s, axis=0, keepdims=True)
        for h in range(CORES):
            own_s[lax.rem(b, 4), h] = s[:, h * HALF:(h + 1) * HALF]
        st_pair(b).start()

    def backward(b):
        sl4 = lax.rem(b, 4)
        st_back(b).wait_recv()
        sl3 = lax.rem(b, 3)
        for h in range(CORES):
            s = Sb[sl4, h]
            s_out[b, :, h * HALF:(h + 1) * HALF] = s
            svec[:, h * HALF:(h + 1) * HALF] = 1.0 / (s * total)
        tl = tls[sl3]
        t1 = jnp.sum(tl, axis=0, keepdims=True)
        at_label = (1.0 - t1 * t1) * (1.0 / total)
        hit = lax.broadcasted_iota(jnp.int32, (V, TB), 0) == labm[sl3]
        dz = (U[sl3, pl.ds(0, V), :] * svec[...] - jnp.where(hit, at_label, 0.0)).astype(BF16)
        sl = lax.rem(b, 2)
        dnb[sl, pl.ds(0, D), :] = jnp.dot(WT[...], dz, preferred_element_type=F32)
        dnb[sl, pl.ds(D, PAD_ROWS), :] = tl
        dW[...] += lax.dot_general(nblk[sl4], dz, (((1,), (1,)), ((), ())), preferred_element_type=F32)
        for keep, give in dn_moves(b):
            keep.start()
            give.start()
        st_pair(b).wait_send()
        for k in range(1, nz):
            st_chip(b, k).wait_send()
        st_back(b).wait_send()

    def finish_tile(sb, acc):
        dn = acc[0:D]
        h = hid_tile(sb)
        r = rinv[sb]
        xhat = h * r
        dgacc[...] += dn * xhat
        dx = dn * gain[...]
        m = jnp.mean(dx * xhat, axis=0, keepdims=True)
        dh[sb // per_mb, :, mb_lanes(sb)] = (
            r * (dx - xhat * m)).astype(BF16)
        own_s = s_out[sb * per_sb + me // TILES, :, pl.ds(pl.multiple_of(lax.rem(me, TILES) * LANE, LANE), LANE)]
        loss = jnp.log(own_s) - SOFT_CAP * jnp.sum(acc[D:D8], axis=0, keepdims=True)
        for m in range(hid.shape[0]):
            @pl.when(sb // per_mb == m)
            def _():
                loss_out[m:m + 1, mb_lanes(sb)] = loss
        lacc[...] += loss

    RS0 = per_sb + 2
    n_rs = nsb - 1

    def first_sent():
        for p in range(PIECES):
            for d in (0, 1):
                for r in range(HOPS[d]):
                    first_ring(d, r, p).wait_send()
            for d, r in FIRSTP:
                first_partner(d, r, p).wait_send()

    def step(s, _):
        @pl.when(s == 2)
        def _():
            first_sent()

        @pl.when((s >= 1) & (s - 1 < nb))
        def _():
            b = s - 1
            sl = lax.rem(b, 4)
            st_pair(b).wait_recv()
            x2[sl, z] = own_s[sl, core] + x1[sl]
            for k in range(1, nz):
                st_chip(b, k).start()

        ring_step(s - 1 - RS0, 1)

        @pl.when((s >= 2) & (s - 2 < nb))
        def _():
            b = s - 2
            sl = lax.rem(b, 4)
            for k in range(1, nz):
                st_chip(b, k).wait_recv()
            acc = x2[sl, 0]
            for k in range(1, nz):
                acc = acc + x2[sl, k]
            Sb[sl, core] = acc
            st_back(b).start()

        if nsb > 1:
            for r in range(HOPS[0], 0, -1):
                @pl.when(s == r - 1)
                def _():
                    ag_next(1, r)
        for r in range(HOPS[0], -1, -1):
            u = s - 2 * r
            sb = jnp.where(u <= 3, (u + 5) // 2, 5 + (u - 6) // 5)
            now = ((u >= -1) & (u <= 3) & (lax.rem(u + 1, 2) == 0)) | ((u >= 6) & (lax.rem(u - 6, 5) == 0))

            @pl.when(now & (sb < nsb))
            def _():
                if r == 0:
                    ag_first(sb)
                else:
                    ag_next(sb, r)

        @pl.when((lax.rem(s + 1, per_sb) == 0) & (s + 1 < nb))
        def _():
            ag_wait((s + 1) // per_sb)

        @pl.when((s + 1 >= per_sb) & (s + 1 < nb))
        def _():
            for c in n_loads(s + 1):
                c.start()

        @pl.when((s >= 4) & (s - 4 < nb) & (lax.rem(s, per_sb) != per_sb - 1))
        def _():
            for keep, give in dn_moves(s - 4):
                keep.wait()
                give.wait_send()

        q = s - RS0
        rsb, r = q // per_sb, lax.rem(q, per_sb)

        def ring_loads():
            for d in (0, 1):
                @pl.when(r < HOPS[d])
                def _():
                    for c in tile_loads(rsb, ring_target(rsb, d, r), d):
                        c.start()

        @pl.when((q >= 0) & (rsb < n_rs) & (r > 0))
        def _():
            ring_loads()

        last = (q >= per_sb) & (r == 0) & (rsb <= n_rs)

        @pl.when(last)
        def _():
            for c in tile_loads(rsb - 1, z, 2):
                c.start()

        @pl.when(s < nb)
        def _():
            forward(s)

        @pl.when((q >= 0) & (rsb < n_rs) & (r == 0))
        def _():
            for keep, give in dn_moves(s - 3):
                keep.wait()
                give.wait_send()

            def body(i, _):
                prx_arrived(rsb, i)
                return 0
            lax.fori_loop(0, nz, body, 0)
            ring_loads()

        ring_step(q, 0)

        @pl.when((s >= 2) & (s - 2 < nb))
        def _():
            backward(s - 2)

        @pl.when(last)
        def _():
            own_tile(rsb - 1)
        return 0
    n_steps = RS0 + n_rs * per_sb
    lax.fori_loop(0, n_steps, step, 0)

    sb = nsb - 1
    par = sb % 2
    assert n_steps == nb + 2
    w_store = pltpu.make_async_copy(dW, dW_out, io_sem.at[0])
    w_store.start()
    ring_step(jnp.int32(n_steps - 1 - RS0), 1)
    for b in range(nb - 2, nb):
        for keep, give in dn_moves(b):
            keep.wait()
            give.wait_send()

    def prx_wait(i, _):
        prx_arrived(sb, i)
        return 0
    lax.fori_loop(0, nz, prx_wait, 0)

    def slot(half, e):
        return U.at[half, pl.ds(e // 4 * D8, D8), pl.ds(e % 4 * LANE, LANE)]

    hops = [(d, r) for r in range(HOPS[0]) for d in (0, 1) if r < HOPS[d]]
    loads = []
    for e, chip in enumerate([ring_target(sb, d, r) for d, r in hops] + [z]):
        chip = lax.rem(chip + 2 * nz, nz)
        loads.append([pltpu.make_async_copy(dnp.at[sb, chip], slot(0, e), tl_sem.at[0, e]),
                      pltpu.make_async_copy(prx.at[sb, chip], slot(1, e), tl_sem.at[1, e])])
        for c in loads[-1]:
            c.start()
    cuts = [D8 // 8 * p // PIECES * 8 for p in range(PIECES + 1)]

    def piece(p):
        return pl.ds(cuts[p], cuts[p + 1] - cuts[p])

    def tail_copy(e, p):
        d, r = hops[e]
        return remote(slot(0, e).at[piece(p)], rx.at[par, d * HOPS[0] + r, piece(p)],
                      tail_send.at[e, p], tail_recv.at[d * HOPS[0] + r, p], at(dev(z + sign(sb, d))))

    def tail_arrived(d, r, p):
        remote(slot(0, 0).at[piece(p)], rx.at[par, d * HOPS[0] + r, piece(p)], tail_send.at[0, p],
               tail_recv.at[d * HOPS[0] + r, p], partner).wait_recv()

    if n_rs > 0:
        for c in tile_loads(n_rs - 1, z, 2):
            c.start()
    def old_sends():
        for k in range(1, n_pp):
            lab_copy(k).wait_send()

        def finish(sb, _):
            for d in (0, 1):
                for r in range(HOPS[d]):
                    ag_ring(sb, d, r).wait_send()

            def body(i, _):
                ag_partner(sb, i).wait_send()
                return 0
            lax.fori_loop(0, nz, body, 0)
            return 0
        lax.fori_loop(1, nsb, finish, 0)

    for e, (d, r) in enumerate(hops):
        if r == 1 and d == 0:
            old_sends()
        if r == 1 and d == 0 and n_rs > 0:
            for h in (0, 1):
                ring_step(jnp.int32(n_rs * per_sb), h)
            own_tile(n_rs - 1)
        for c in loads[e]:
            c.wait()
        for p in range(PIECES):
            mine, other = slot(0, e).at[piece(p)], slot(1, e).at[piece(p)]
            if r > 0:
                tail_arrived(d, r - 1, p)
                mine[...] = mine[...] + other[...] + rx[par, d * HOPS[0] + r - 1, piece(p)]
            else:
                mine[...] = mine[...] + other[...]
            tail_copy(e, p).start()
    for c in loads[len(hops)]:
        c.wait()
    for d in (0, 1):
        for p in range(PIECES):
            tail_arrived(d, HOPS[d] - 1, p)
    finish_tile(sb, slot(0, len(hops))[...] + slot(1, len(hops))[...] + rx[par, HOPS[0] - 1]
                + rx[par, HOPS[0] + HOPS[1] - 1])

    ex_own[:, 0:D] = jnp.sum(dgacc[...].T, axis=0, keepdims=True)
    ex_own[:, pl.ds(ex_own.shape[1] - LANE, LANE)] = lacc[...]
    exs = [remote(ex_own, ex_rx.at[me], ex_send.at[k - 1], ex_recv.at[n_pp - 1 - k], at(lax.rem(me + k, n_pp)))
           for k in range(1, n_pp)]
    for c in exs:
        c.start()
    for c in exs:
        c.wait_recv()
    acc = jnp.zeros_like(ex_out)
    for k in range(n_pp):
        acc = acc + jnp.where(k == me, ex_own[...], ex_rx[k])
    ex_out[...] = acc
    for c in exs:
        c.wait_send()
    for e in range(len(hops)):
        for p in range(PIECES):
            tail_copy(e, p).wait_send()
    w_store.wait()


def mega_call(hid, lab_own, gamma, WT, *, n_pp, total, cid=1):
    mb, D, seq = hid.shape
    T = mb * seq
    V = WT.shape[1]
    D8, nz, nsb = D + PAD_ROWS, n_pp // CORES, T // LANE
    nb = nsb * n_pp // TILES
    EX = -(-D // LANE) * LANE + LANE
    hbm, vmem = pl.BlockSpec(memory_space=pl.ANY), pl.BlockSpec(memory_space=pltpu.VMEM)
    dma, sd = pltpu.SemaphoreType.DMA, jax.ShapeDtypeStruct
    out = pl.pallas_call(
        functools.partial(kernel, n_pp, float(total)),
        out_shape=[sd((mb, D, seq), BF16), sd((D, V), F32), sd((mb, seq), F32), sd((1, EX), F32),
                   sd((n_pp, D, T), BF16), sd((nsb, nz, D8, LANE), F32), sd((nsb, nz, D8, LANE), F32)],
        in_specs=[vmem] * 4,
        out_specs=[vmem, hbm, vmem, vmem, hbm, hbm, hbm],
        scratch_shapes=[
            pltpu.VMEM((D, T), BF16), pltpu.VMEM((V, D), BF16), pltpu.VMEM((D, LANE), F32), pltpu.VMEM((nsb, 1, LANE), F32),
            pltpu.VMEM((D, LANE), F32), pltpu.VMEM((1, LANE), F32), pltpu.VMEM((nb, 1, TB), F32),
            pltpu.VMEM((1, EX), F32), pltpu.VMEM((n_pp, 1, EX), F32),
            pltpu.VMEM((3, max(V, 2 * D8), TB), F32), pltpu.VMEM((4, D, TB), BF16), pltpu.VMEM((D, V), F32),
            pltpu.VMEM((2, D8, TB), F32), pltpu.VMEM((1, TB), F32), pltpu.VMEM((3, 1, TB), jnp.int32),
            pltpu.VMEM((3, 8, TB), F32),
            pltpu.VMEM((n_pp, mb, seq), jnp.int32), pltpu.VMEM((4, CORES, 1, HALF), F32), pltpu.VMEM((4, 1, HALF), F32),
            pltpu.VMEM((4, nz, 1, HALF), F32), pltpu.VMEM((4, CORES, 1, HALF), F32),
            pltpu.VMEM((2, sum(HOPS), D8, LANE), F32), pltpu.VMEM((3, 2, D8, LANE), F32),
            pltpu.VMEM((2, D8, LANE), F32),
            dma((nsb, 2, HOPS[0])), dma((nsb, 2, HOPS[0])), dma((nsb, nz)), dma((nsb, nz)),
            dma((nsb, nz)), dma((2, 2)), dma((2, 2)), dma((2, sum(HOPS), 2)), dma((2, 2)),
            dma((4, nz + 1)), dma((4, nz + 1)), dma((n_pp - 1,)), dma((n_pp - 1,)), dma((4, TILES)), dma((3, 2)), dma((1,)),
            dma((sum(HOPS), PIECES)), dma((sum(HOPS), PIECES)), dma((2, sum(HOPS) + 1)),
            dma((n_pp - 1,)), dma((n_pp - 1,)),
            *[dma((2, HOPS[0] + 1, PIECES))] * 4,
        ],
        compiler_params=pltpu.CompilerParams(vmem_limit_bytes=63 * 1024 * 1024, collective_id=cid, has_side_effects=True),
        cost_estimate=pl.CostEstimate(flops=6 * n_pp * T * D * V, bytes_accessed=n_pp * T * D * 20, transcendentals=0),
        name="head")(hid, lab_own, gamma, WT)
    return out[:4]


def solution(mesh):
    n_pp = mesh.shape["pp"]

    def local_fn(hidden, labels, gamma, table):
        mb, seq, D = hidden.shape
        V = table.shape[0]
        T = mb * seq
        total = T * n_pp
        dh, dW, loss, sums = mega_call(jnp.swapaxes(hidden, 1, 2), labels, gamma.reshape(1, D), table.T,
                                       n_pp=n_pp, total=total)
        return (loss, jnp.swapaxes(dh, 1, 2), jnp.sum(sums[0, -LANE:])[None] / total, dW.T, sums[0, :D])

    token_spec = P(("dp", "pp"))
    return jax.shard_map(local_fn, mesh=mesh,
                         in_specs=(token_spec, token_spec, P(), P("pp")),
                         out_specs=(token_spec, token_spec, P("dp"), token_spec, P("dp")),
                         check_vma=False)
```

```python
import functools
import math

import jax
import jax.numpy as jnp
from jax import lax
from jax.experimental import pallas as pl
from jax.experimental.pallas import tpu as pltpu
from jax.sharding import PartitionSpec as P

F32, BF16 = jnp.float32, jnp.bfloat16
SOFT_CAP = 30.0
EPS = 1e-6
EXP2_SCALE = SOFT_CAP * math.log2(math.e)
MESH = pl.DeviceIdType.MESH
CORES = 2
LANE = 128
TILES = 4
TB = LANE * TILES
HALF = TB // CORES
PAD_ROWS = 8
PIECES = 4
TAIL_PIECES = 6
WROWS = 256
FWD_PARTS = 24
HOPS = (4, 3)


def kernel(n_pp, total, hid, lab_own, gamma, WT,
           dh, dW_out, loss_out, ex_out, n_all, dnp, prx,
           n_own, W, gain, rinv, dgacc, lacc, s_out, ex_own, ex_rx,
           U, nblk, dW, dnb, svec, labm, tls, lab_all, own_s, x1, x2, Sb, rx, ownv, sendb,
           ag_recv, ag_send, pag_recv, pag_send, pair_recv, pair_send, dnp_sem, ring_recv, ring_send,
           st_recv, st_send, lab_recv, lab_send, nl_sem, ov_sem, io_sem, tail_recv, tail_send, tl_sem, ex_recv, ex_send,
           first_recv, first_send, firstp_recv, firstp_send):
    D, T = n_own.shape
    V = W.shape[0]
    seq = hid.shape[2]
    per_mb = seq // LANE
    wrows = min(WROWS, V)
    D8 = D + PAD_ROWS
    nz = n_pp // CORES
    nsb = T // LANE
    per_sb = n_pp // TILES
    nb = nsb * per_sb
    me = lax.axis_index("pp")
    z, core = me // CORES, lax.rem(me, CORES)

    def dev(chip, c=core):
        return lax.rem(chip + 2 * nz, nz) * CORES + c

    def at(index):
        return {"pp": index}

    partner = at(z * CORES + 1 - core)

    def lanes_of(sb):
        return pl.ds(pl.multiple_of(sb * LANE, LANE), LANE)

    def remote(src, dst, ssem, rsem, where):
        return pltpu.make_async_remote_copy(src_ref=src, dst_ref=dst, send_sem=ssem, recv_sem=rsem,
                                            device_id=where, device_id_type=MESH)

    def mb_lanes(sb):
        return pl.ds(pl.multiple_of(lax.rem(sb, per_mb) * LANE, LANE), LANE)

    def sign(sb, d):
        g = 1 - 2 * lax.rem(sb, 2)
        return g if d == 0 else -g

    def ag_ring(sb, d, r):
        g = sign(sb, d)
        if r == 0:
            src = n_own.at[:, lanes_of(sb)]
        else:
            src = n_all.at[dev(z - g * r), :, lanes_of(sb)]
        return remote(src, n_all.at[dev(z - g * r), :, lanes_of(sb)], ag_send.at[sb, d, r], ag_recv.at[sb, d, r],
                      at(dev(z + g)))

    def ag_partner(sb, chip, own=False):
        i = lax.rem(chip + 2 * nz, nz)
        src = n_own.at[:, lanes_of(sb)] if own else n_all.at[dev(chip), :, lanes_of(sb)]
        return remote(src, n_all.at[dev(chip), :, lanes_of(sb)], pag_send.at[sb, i], pag_recv.at[sb, i], partner)

    rows0 = D // PIECES

    def first_tile(chip, p):
        i = dev(chip)
        return nblk.at[i // TILES, pl.ds(p * rows0, rows0), pl.ds(pl.multiple_of(lax.rem(i, TILES) * LANE, LANE), LANE)]

    def first_ring(d, r, p):
        g = sign(0, d)
        ref = first_tile(z - g * r, p)
        return remote(ref, ref, first_send.at[d, r, p], first_recv.at[d, r, p], at(dev(z + g)))

    def first_partner(d, r, p):
        ref = first_tile(z - sign(0, d) * r, p)
        return remote(ref, ref, firstp_send.at[d, r, p], firstp_recv.at[d, r, p], partner)

    FIRSTP = [(d, r) for r in range(HOPS[0] + 1) for d in (0, 1) if r <= HOPS[d] and (r, d) != (0, 1)]

    def ag_first(sb):
        for d in (0, 1):
            ag_ring(sb, d, 0).start()
        ag_partner(sb, z, own=True).start()

    def ag_next(sb, r):
        for d in (0, 1):
            if r <= HOPS[d]:
                ag_ring(sb, d, r - 1).wait_recv()
                if r < HOPS[d]:
                    ag_ring(sb, d, r).start()
                ag_partner(sb, z - sign(sb, d) * r).start()

    def ag_wait(sb):
        def body(i, _):
            ag_partner(sb, i).wait_recv()
            return 0
        lax.fori_loop(0, nz, body, 0)

    def n_loads(b):
        sb, j = b // per_sb, lax.rem(b, per_sb)
        return [pltpu.make_async_copy(n_all.at[j * TILES + a, :, lanes_of(sb)],
                                      nblk.at[lax.rem(b, 4), :, pl.ds(a * LANE, LANE)],
                                      nl_sem.at[lax.rem(b, 4), a]) for a in range(TILES)]

    def dn_moves(b):
        sb, j, sl = b // per_sb, lax.rem(b, per_sb), lax.rem(b, 2)
        out = []
        for h in range(TILES // CORES):
            chip = j * (TILES // CORES) + h
            here = pl.ds(pl.multiple_of((h * CORES + core) * LANE, LANE), LANE)
            there = pl.ds(pl.multiple_of((h * CORES + 1 - core) * LANE, LANE), LANE)
            out.append((pltpu.make_async_copy(dnb.at[sl, :, here], dnp.at[sb, chip], dnp_sem.at[sl, h]),
                        remote(dnb.at[sl, :, there], prx.at[sb, chip], pair_send.at[sl, h],
                               pair_recv.at[sb, chip], partner)))
        return out

    def prx_arrived(sb, i):
        remote(dnb.at[0, :, pl.ds(0, LANE)], prx.at[sb, i], pair_send.at[0, 0], pair_recv.at[sb, i],
               partner).wait_recv()

    def tile_loads(sb, chip, k):
        chip = lax.rem(chip + 2 * nz, nz)
        return [pltpu.make_async_copy(dnp.at[sb, chip], ownv.at[k, 0], ov_sem.at[k, 0]),
                pltpu.make_async_copy(prx.at[sb, chip], ownv.at[k, 1], ov_sem.at[k, 1])]

    def rx_slot(sb, d, r):
        return rx.at[lax.rem(sb, 2), d * HOPS[0] + r]

    cut = D8 // 16 * 8
    part = (pl.ds(0, cut), pl.ds(cut, D8 - cut))

    def ring_copy(sb, d, r, h):
        return remote(sendb.at[d, part[h]], rx_slot(sb, d, r).at[part[h]], ring_send.at[d, h],
                      ring_recv.at[lax.rem(sb, 2), d * HOPS[0] + r, h], at(dev(z + sign(sb, d))))

    def ring_step(q, h):
        sb, r = q // per_sb, lax.rem(q, per_sb)
        for d in (0, 1):
            @pl.when((q >= 1) & (q - 1 < n_rs * per_sb) & (lax.rem(q - 1, per_sb) < HOPS[d]))
            def _():
                ring_copy((q - 1) // per_sb, d, lax.rem(q - 1, per_sb), h).wait_send()

            @pl.when((q >= 0) & (sb < n_rs) & (r < HOPS[d]))
            def _():
                if h == 0:
                    for c in tile_loads(sb, ring_target(sb, d, r), d):
                        c.wait()

                @pl.when(r == 0)
                def _():
                    sendb[d, part[h], :] = ownv[d, 0, part[h], :] + ownv[d, 1, part[h], :]

                @pl.when(r > 0)
                def _():
                    ring_copy(sb, d, r - 1, h).wait_recv()
                    sendb[d, part[h], :] = (ownv[d, 0, part[h], :] + ownv[d, 1, part[h], :]
                                            + rx[lax.rem(sb, 2), d * HOPS[0] + r - 1, part[h], :])
                ring_copy(sb, d, r, h).start()

    def own_tile(sb):
        for c in tile_loads(sb, z, 2):
            c.wait()
        for d in (0, 1):
            for h in (0, 1):
                ring_copy(sb, d, HOPS[d] - 1, h).wait_recv()
        acc = ownv[2, 0] + ownv[2, 1]
        for d in (0, 1):
            acc = acc + rx[lax.rem(sb, 2), d * HOPS[0] + HOPS[d] - 1]
        finish_tile(sb, acc)

    def ring_target(sb, d, r):
        return z + sign(sb, d) * (HOPS[d] - r)

    def st_pair(b):
        sl = lax.rem(b, 4)
        return remote(own_s.at[sl, 1 - core], x1.at[sl], st_send.at[sl, 0], st_recv.at[sl, 0], partner)

    def st_chip(b, k):
        sl = lax.rem(b, 4)
        return remote(x2.at[sl, z], x2.at[sl, z], st_send.at[sl, k], st_recv.at[sl, nz - k], at(dev(z + k)))

    def st_back(b):
        sl = lax.rem(b, 4)
        return remote(Sb.at[sl, core], Sb.at[sl, core], st_send.at[sl, nz], st_recv.at[sl, nz], partner)

    def lab_copy(k):
        return remote(lab_own, lab_all.at[me], lab_send.at[k - 1], lab_recv.at[n_pp - 1 - k],
                      at(lax.rem(me + k, n_pp)))

    def hid_tile(sb):
        return hid[sb // per_mb, :, mb_lanes(sb)].astype(F32)

    def norm_tile(sb):
        h = hid_tile(sb)
        r = lax.rsqrt(jnp.mean(h * h, axis=0, keepdims=True) + EPS)
        rinv[sb] = r
        n_own[:, lanes_of(sb)] = (h * r * gain[...]).astype(BF16)

    def turn_table(c):
        rows = pl.ds(pl.multiple_of(c * wrows, wrows), wrows)
        W[rows, :] = WT[:, rows].T

    barrier = pltpu.get_barrier_semaphore()
    for k in range(1, n_pp):
        pl.semaphore_signal(barrier, inc=1, device_id=at(lax.rem(me + k, n_pp)), device_id_type=MESH)
    gain[...] = jnp.broadcast_to(1.0 + gamma[...], (LANE, D)).T
    norm_tile(0)
    for p in range(PIECES):
        first_tile(z, p)[...] = n_own[p * rows0:(p + 1) * rows0, 0:LANE]
    pl.semaphore_wait(barrier, n_pp - 1)
    for p in range(PIECES):
        for d in (0, 1):
            first_ring(d, 0, p).start()
        first_partner(0, 0, p).start()
    for k in range(1, n_pp):
        lab_copy(k).start()
    lab_all[me] = lab_own[...]

    def rest(sb, _):
        norm_tile(sb)
        return 0
    lax.fori_loop(1, nsb, rest, 0)
    own_copy = pltpu.make_async_copy(n_own, n_all.at[me], io_sem.at[0])
    own_copy.start()
    dW[...] = jnp.zeros_like(dW)
    dgacc[...] = jnp.zeros_like(dgacc)
    lacc[...] = jnp.zeros_like(lacc)
    n_turn = V // wrows
    for r in range(1, HOPS[0] + 1):
        def turn(c, _):
            turn_table(c)
            return 0
        lax.fori_loop(n_turn * (r - 1) // HOPS[0], n_turn * r // HOPS[0], turn, 0)
        for p in range(PIECES):
            for d in (0, 1):
                if r <= HOPS[d]:
                    first_ring(d, r - 1, p).wait_recv()
                    if r < HOPS[d]:
                        first_ring(d, r, p).start()
                    first_partner(d, r, p).start()
        if r == HOPS[0] - 1 and nsb > 1:
            ag_first(1)
    if nsb > 2:
        ag_first(2)
    own_copy.wait()
    for d, r in FIRSTP:
        for p in range(PIECES):
            first_partner(d, r, p).wait_recv()
    for k in range(1, n_pp):
        lab_copy(k).wait_recv()

    base = me * V

    def forward(b):
        @pl.when(b >= per_sb)
        def _():
            for c in n_loads(b):
                c.wait()
        sl3 = lax.rem(b, 3)
        sb, j = b // per_sb, lax.rem(b, per_sb)
        for a in range(TILES):
            rows = lab_all[j * TILES + a, :, mb_lanes(sb)]
            row = rows[0:1]
            for m in range(1, rows.shape[0]):
                row = jnp.where(sb // per_mb == m, rows[m:m + 1], row)
            labm[sl3, :, a * LANE:(a + 1) * LANE] = row - base
        s = jnp.zeros((8, TB), F32)
        tl = jnp.zeros((8, TB), F32)
        n = V // FWD_PARTS
        for c in range(FWD_PARTS):
            zl = jnp.dot(W[c * n:(c + 1) * n, :], nblk[lax.rem(b, 4)], preferred_element_type=F32)
            t = jnp.tanh(zl * (1.0 / SOFT_CAP))
            e = jnp.exp2(t * EXP2_SCALE)
            U[sl3, c * n:(c + 1) * n, :] = e * (1.0 - t * t)
            hit = lax.broadcasted_iota(jnp.int32, (n, TB), 0) == labm[sl3] - c * n
            s = s + jnp.sum(e.reshape(n // 8, 8, TB), axis=0)
            tl = tl + jnp.sum(jnp.where(hit, t, 0.0).reshape(n // 8, 8, TB), axis=0)
        tls[sl3] = tl
        s = jnp.sum(s, axis=0, keepdims=True)
        for h in range(CORES):
            own_s[lax.rem(b, 4), h] = s[:, h * HALF:(h + 1) * HALF]
        st_pair(b).start()

    def backward(b):
        sl4 = lax.rem(b, 4)
        st_back(b).wait_recv()
        sl3 = lax.rem(b, 3)
        for h in range(CORES):
            s = Sb[sl4, h]
            s_out[b, :, h * HALF:(h + 1) * HALF] = s
            svec[:, h * HALF:(h + 1) * HALF] = 1.0 / (s * total)
        tl = tls[sl3]
        t1 = jnp.sum(tl, axis=0, keepdims=True)
        at_label = (1.0 - t1 * t1) * (1.0 / total)
        hit = lax.broadcasted_iota(jnp.int32, (V, TB), 0) == labm[sl3]
        dz = (U[sl3, pl.ds(0, V), :] * svec[...] - jnp.where(hit, at_label, 0.0)).astype(BF16)
        sl = lax.rem(b, 2)
        dnb[sl, pl.ds(0, D), :] = jnp.dot(WT[...], dz, preferred_element_type=F32)
        dnb[sl, pl.ds(D, PAD_ROWS), :] = tl
        for keep, give in dn_moves(b):
            keep.start()
            give.start()
        dW[...] += lax.dot_general(nblk[sl4], dz, (((1,), (1,)), ((), ())), preferred_element_type=F32)
        st_pair(b).wait_send()
        for k in range(1, nz):
            st_chip(b, k).wait_send()
        st_back(b).wait_send()

    def finish_tile(sb, acc):
        dn = acc[0:D]
        h = hid_tile(sb)
        r = rinv[sb]
        xhat = h * r
        dgacc[...] += dn * xhat
        dx = dn * gain[...]
        m = jnp.mean(dx * xhat, axis=0, keepdims=True)
        dh[sb // per_mb, :, mb_lanes(sb)] = (
            r * (dx - xhat * m)).astype(BF16)
        own_s = s_out[sb * per_sb + me // TILES, :, pl.ds(pl.multiple_of(lax.rem(me, TILES) * LANE, LANE), LANE)]
        loss = jnp.log(own_s) - SOFT_CAP * jnp.sum(acc[D:D8], axis=0, keepdims=True)
        for m in range(hid.shape[0]):
            @pl.when(sb // per_mb == m)
            def _():
                loss_out[m:m + 1, mb_lanes(sb)] = loss
        lacc[...] += loss

    RS0 = per_sb + 2
    n_rs = nsb - 1

    def first_sent():
        for p in range(PIECES):
            for d in (0, 1):
                for r in range(HOPS[d]):
                    first_ring(d, r, p).wait_send()
            for d, r in FIRSTP:
                first_partner(d, r, p).wait_send()

    def step(s, _):
        @pl.when(s == 2)
        def _():
            first_sent()

        @pl.when((s >= 1) & (s - 1 < nb))
        def _():
            b = s - 1
            sl = lax.rem(b, 4)
            st_pair(b).wait_recv()
            x2[sl, z] = own_s[sl, core] + x1[sl]
            for k in range(1, nz):
                st_chip(b, k).start()

        ring_step(s - 1 - RS0, 1)

        @pl.when((s >= 2) & (s - 2 < nb))
        def _():
            b = s - 2
            sl = lax.rem(b, 4)
            for k in range(1, nz):
                st_chip(b, k).wait_recv()
            acc = x2[sl, 0]
            for k in range(1, nz):
                acc = acc + x2[sl, k]
            Sb[sl, core] = acc
            st_back(b).start()

        if nsb > 1:
            @pl.when(s == HOPS[0] - 1)
            def _():
                ag_next(1, HOPS[0])
        for r in range(HOPS[0], -1, -1):
            u = s - 2 * r
            sb = jnp.where(u <= 0, u + 3, jnp.where(u <= 4, u + 1, 6 + (u - 9) // 5))
            now = ((u >= -1) & (u <= 0)) | ((u >= 3) & (u <= 4)) | ((u >= 9) & (lax.rem(u - 9, 5) == 0))

            @pl.when(now & (sb < nsb))
            def _():
                if r == 0:
                    ag_first(sb)
                else:
                    ag_next(sb, r)

        @pl.when((lax.rem(s + 1, per_sb) == 0) & (s + 1 < nb))
        def _():
            ag_wait((s + 1) // per_sb)

        @pl.when((s + 1 >= per_sb) & (s + 1 < nb))
        def _():
            for c in n_loads(s + 1):
                c.start()

        @pl.when((s >= 4) & (s - 4 < nb) & (lax.rem(s, per_sb) != per_sb - 1))
        def _():
            for keep, give in dn_moves(s - 4):
                keep.wait()
                give.wait_send()

        q = s - RS0
        rsb, r = q // per_sb, lax.rem(q, per_sb)

        def ring_loads():
            for d in (0, 1):
                @pl.when(r < HOPS[d])
                def _():
                    for c in tile_loads(rsb, ring_target(rsb, d, r), d):
                        c.start()

        @pl.when((q >= 0) & (rsb < n_rs) & (r > 0))
        def _():
            ring_loads()

        last = (q >= per_sb) & (r == 0) & (rsb <= n_rs)

        @pl.when(last)
        def _():
            for c in tile_loads(rsb - 1, z, 2):
                c.start()

        @pl.when((q >= 0) & (rsb < n_rs) & (r == 0))
        def _():
            for keep, give in dn_moves(s - 3):
                keep.wait()
                give.wait_send()

            def body(i, _):
                prx_arrived(rsb, i)
                return 0
            lax.fori_loop(0, nz, body, 0)
            ring_loads()

        @pl.when(s < nb)
        def _():
            forward(s)

        ring_step(q, 0)

        if nsb > 1:
            for r in range(HOPS[0] - 1, 0, -1):
                @pl.when(s == r - 1)
                def _():
                    ag_next(1, r)

        @pl.when((s >= 2) & (s - 2 < nb))
        def _():
            backward(s - 2)

        @pl.when(last)
        def _():
            own_tile(rsb - 1)
        return 0
    n_steps = RS0 + n_rs * per_sb
    lax.fori_loop(0, n_steps, step, 0)

    sb = nsb - 1
    par = sb % 2
    assert n_steps == nb + 2
    w_store = pltpu.make_async_copy(dW, dW_out, io_sem.at[0])
    w_store.start()
    ring_step(jnp.int32(n_steps - 1 - RS0), 1)
    for b in range(nb - 2, nb):
        for keep, give in dn_moves(b):
            keep.wait()
            give.wait_send()

    def prx_wait(i, _):
        prx_arrived(sb, i)
        return 0
    lax.fori_loop(0, nz, prx_wait, 0)

    def slot(half, e):
        return U.at[half, pl.ds(e // 4 * D8, D8), pl.ds(e % 4 * LANE, LANE)]

    hops = [(d, r) for r in range(HOPS[0]) for d in (0, 1) if r < HOPS[d]]
    loads = []
    for e, chip in enumerate([ring_target(sb, d, r) for d, r in hops] + [z]):
        chip = lax.rem(chip + 2 * nz, nz)
        loads.append([pltpu.make_async_copy(dnp.at[sb, chip], slot(0, e), tl_sem.at[0, e]),
                      pltpu.make_async_copy(prx.at[sb, chip], slot(1, e), tl_sem.at[1, e])])
        for c in loads[-1]:
            c.start()
    cuts = [D8 // 8 * p // TAIL_PIECES * 8 for p in range(TAIL_PIECES + 1)]

    def piece(p):
        return pl.ds(cuts[p], cuts[p + 1] - cuts[p])

    def tail_copy(e, p):
        d, r = hops[e]
        return remote(slot(0, e).at[piece(p)], rx.at[par, d * HOPS[0] + r, piece(p)],
                      tail_send.at[e, p], tail_recv.at[d * HOPS[0] + r, p], at(dev(z + sign(sb, d))))

    def tail_arrived(d, r, p):
        remote(slot(0, 0).at[piece(p)], rx.at[par, d * HOPS[0] + r, piece(p)], tail_send.at[0, p],
               tail_recv.at[d * HOPS[0] + r, p], partner).wait_recv()

    if n_rs > 0:
        for c in tile_loads(n_rs - 1, z, 2):
            c.start()
    def old_sends():
        for k in range(1, n_pp):
            lab_copy(k).wait_send()

        def finish(sb, _):
            for d in (0, 1):
                for r in range(HOPS[d]):
                    ag_ring(sb, d, r).wait_send()

            def body(i, _):
                ag_partner(sb, i).wait_send()
                return 0
            lax.fori_loop(0, nz, body, 0)
            return 0
        lax.fori_loop(1, nsb, finish, 0)

    for e, (d, r) in enumerate(hops):
        if r == 1 and d == 0:
            old_sends()
        if r == 1 and d == 0 and n_rs > 0:
            for h in (0, 1):
                ring_step(jnp.int32(n_rs * per_sb), h)
            own_tile(n_rs - 1)
        for c in loads[e]:
            c.wait()
        for p in range(TAIL_PIECES):
            mine, other = slot(0, e).at[piece(p)], slot(1, e).at[piece(p)]
            if r > 0:
                tail_arrived(d, r - 1, p)
                mine[...] = mine[...] + other[...] + rx[par, d * HOPS[0] + r - 1, piece(p)]
            else:
                mine[...] = mine[...] + other[...]
            tail_copy(e, p).start()
    for c in loads[len(hops)]:
        c.wait()
    for d in (0, 1):
        for p in range(TAIL_PIECES):
            tail_arrived(d, HOPS[d] - 1, p)
    finish_tile(sb, slot(0, len(hops))[...] + slot(1, len(hops))[...] + rx[par, HOPS[0] - 1]
                + rx[par, HOPS[0] + HOPS[1] - 1])

    ex_own[:, 0:D] = jnp.sum(dgacc[...].T, axis=0, keepdims=True)
    ex_own[:, pl.ds(ex_own.shape[1] - LANE, LANE)] = lacc[...]
    exs = [remote(ex_own, ex_rx.at[me], ex_send.at[k - 1], ex_recv.at[n_pp - 1 - k], at(lax.rem(me + k, n_pp)))
           for k in range(1, n_pp)]
    for c in exs:
        c.start()
    for c in exs:
        c.wait_recv()
    acc = jnp.zeros_like(ex_out)
    for k in range(n_pp):
        acc = acc + jnp.where(k == me, ex_own[...], ex_rx[k])
    ex_out[...] = acc
    for c in exs:
        c.wait_send()
    for e in range(len(hops)):
        for p in range(TAIL_PIECES):
            tail_copy(e, p).wait_send()
    w_store.wait()


def mega_call(hid, lab_own, gamma, WT, *, n_pp, total, cid=1):
    mb, D, seq = hid.shape
    T = mb * seq
    V = WT.shape[1]
    D8, nz, nsb = D + PAD_ROWS, n_pp // CORES, T // LANE
    nb = nsb * n_pp // TILES
    EX = -(-D // LANE) * LANE + LANE
    hbm, vmem = pl.BlockSpec(memory_space=pl.ANY), pl.BlockSpec(memory_space=pltpu.VMEM)
    dma, sd = pltpu.SemaphoreType.DMA, jax.ShapeDtypeStruct
    out = pl.pallas_call(
        functools.partial(kernel, n_pp, float(total)),
        out_shape=[sd((mb, D, seq), BF16), sd((D, V), F32), sd((mb, seq), F32), sd((1, EX), F32),
                   sd((n_pp, D, T), BF16), sd((nsb, nz, D8, LANE), F32), sd((nsb, nz, D8, LANE), F32)],
        in_specs=[vmem] * 4,
        out_specs=[vmem, hbm, vmem, vmem, hbm, hbm, hbm],
        scratch_shapes=[
            pltpu.VMEM((D, T), BF16), pltpu.VMEM((V, D), BF16), pltpu.VMEM((D, LANE), F32), pltpu.VMEM((nsb, 1, LANE), F32),
            pltpu.VMEM((D, LANE), F32), pltpu.VMEM((1, LANE), F32), pltpu.VMEM((nb, 1, TB), F32),
            pltpu.VMEM((1, EX), F32), pltpu.VMEM((n_pp, 1, EX), F32),
            pltpu.VMEM((3, max(V, 2 * D8), TB), F32), pltpu.VMEM((4, D, TB), BF16), pltpu.VMEM((D, V), F32),
            pltpu.VMEM((2, D8, TB), F32), pltpu.VMEM((1, TB), F32), pltpu.VMEM((3, 1, TB), jnp.int32),
            pltpu.VMEM((3, 8, TB), F32),
            pltpu.VMEM((n_pp, mb, seq), jnp.int32), pltpu.VMEM((4, CORES, 1, HALF), F32), pltpu.VMEM((4, 1, HALF), F32),
            pltpu.VMEM((4, nz, 1, HALF), F32), pltpu.VMEM((4, CORES, 1, HALF), F32),
            pltpu.VMEM((2, sum(HOPS), D8, LANE), F32), pltpu.VMEM((3, 2, D8, LANE), F32),
            pltpu.VMEM((2, D8, LANE), F32),
            dma((nsb, 2, HOPS[0])), dma((nsb, 2, HOPS[0])), dma((nsb, nz)), dma((nsb, nz)),
            dma((nsb, nz)), dma((2, 2)), dma((2, 2)), dma((2, sum(HOPS), 2)), dma((2, 2)),
            dma((4, nz + 1)), dma((4, nz + 1)), dma((n_pp - 1,)), dma((n_pp - 1,)), dma((4, TILES)), dma((3, 2)), dma((1,)),
            dma((sum(HOPS), TAIL_PIECES)), dma((sum(HOPS), TAIL_PIECES)), dma((2, sum(HOPS) + 1)),
            dma((n_pp - 1,)), dma((n_pp - 1,)),
            *[dma((2, HOPS[0] + 1, PIECES))] * 4,
        ],
        compiler_params=pltpu.CompilerParams(vmem_limit_bytes=63 * 1024 * 1024, collective_id=cid, has_side_effects=True),
        cost_estimate=pl.CostEstimate(flops=6 * n_pp * T * D * V, bytes_accessed=n_pp * T * D * 20, transcendentals=0),
        name="head")(hid, lab_own, gamma, WT)
    return out[:4]


def copy_kernel(parts, a, b, oa, ob, va, vb, sa, sb):
    rows = a.shape[0] // parts
    cut = [pl.ds(i * rows, rows) for i in range(parts)]
    into = [pltpu.make_async_copy(a.at[c], va.at[c], sa.at[0, i]) for i, c in enumerate(cut)]
    away = [pltpu.make_async_copy(va.at[c], oa.at[c], sa.at[1, i]) for i, c in enumerate(cut)]
    into.append(pltpu.make_async_copy(b, vb, sb.at[0]))
    away.append(pltpu.make_async_copy(vb, ob, sb.at[1]))
    for c in into:
        c.start()
    for c, d in zip(into, away):
        c.wait()
        d.start()
    for d in away:
        d.wait()


def own_buffers(a, b, parts=12):
    hbm = pl.BlockSpec(memory_space=pl.ANY)
    sd, dma = jax.ShapeDtypeStruct, pltpu.SemaphoreType.DMA
    return pl.pallas_call(
        functools.partial(copy_kernel, parts), out_shape=[sd(a.shape, a.dtype), sd(b.shape, b.dtype)],
        in_specs=[hbm] * 2, out_specs=[hbm] * 2,
        scratch_shapes=[pltpu.VMEM(a.shape, a.dtype), pltpu.VMEM(b.shape, b.dtype), dma((2, parts)), dma((2,))],
        compiler_params=pltpu.CompilerParams(vmem_limit_bytes=56 * 1024 * 1024), name="own_buffers")(a, b)


def solution(mesh):
    n_pp = mesh.shape["pp"]

    def local_fn(hidden, labels, gamma, table):
        mb, seq, D = hidden.shape
        V = table.shape[0]
        T = mb * seq
        total = T * n_pp
        dh, dW, loss, sums = mega_call(jnp.swapaxes(hidden, 1, 2), labels, gamma.reshape(1, D), table.T,
                                       n_pp=n_pp, total=total)
        dW, dh = own_buffers(dW, dh)
        return (loss, jnp.swapaxes(dh, 1, 2), jnp.sum(sums[0, -LANE:])[None] / total, dW.T, sums[0, :D])

    token_spec = P(("dp", "pp"))
    return jax.shard_map(local_fn, mesh=mesh,
                         in_specs=(token_spec, token_spec, P(), P("pp")),
                         out_specs=(token_spec, token_spec, P("dp"), token_spec, P("dp")),
                         check_vma=False)
```
